1024 devices in a mesh: grp: 64 (over x, z), ep: 16 (over y, core).
Axes of the slice: x: 8, y: 8, z: 8, core: 2. Of those that a mesh axis runs over, the one named last changes fastest.
Arguments:
- out_grad: bfloat16 [8192, 4096], P('grp', 'ep'), may hold values from -6 to 6
- expert_ids: int32 [8192, 8], P('grp'), may hold values from 0 to 127, as said below
- router_logits: float32 [8192, 128], P('grp'), may hold values from -5 to 5
- router_weight: bfloat16 [128, 4096], P(None, 'ep'), may hold values from -0.09375 to 0.09375
- expert_weight: bfloat16 [128, 4096, 1024], P('grp', 'ep'), may hold values from -0.1875 to 0.1875
- hidden_saved: bfloat16 [64, 2048, 1024], P('grp'), may hold values from -6 to 6
Outputs:
- weight_grad: bfloat16 [128, 4096, 1024], P('grp', 'ep')
- hidden_grad: bfloat16 [64, 2048, 1024], P('grp', 'ep')
- input_grad: bfloat16 [8192, 4096], P('grp', 'ep')
The draws below stay inside these ranges and needn't reach their ends.
Inputs may be any that keep to these rules, and one draw needn't show every extreme that they name: `expert_ids`: each row names 8 different experts, lying in at most 4 of the 8 groups of 16 consecutive experts. In each aligned block of 128 rows no expert is named by more than 16 rows, and some expert is named by exactly 16.
All inputs are finite; a program needn't handle non-finite values.
Results may differ from the reference program's by a relative error of at most 0.02.
Values may be sent and summed in bfloat16 or wider, within the bound.
A program may use at most 64 MiB of HBM per device.

```python
import jax
import jax.numpy as jnp
from jax import lax

D = 4096
FF = 1024
EXP_GRP = 2
TOPG = 4
TOPK = 8
EXPERTS = 128
GROUPS = 8
GROUP_EXP = 16
PICK = 2
ROWS_GRP = 128
TOKENS = 8192
USERS = 64
CAP = 16
SLOTS = 2048
N_GRP = 64
N_EP = 16


def draw_expert_ids(key, part):
    group_scores = jax.random.randint(jax.random.fold_in(key, 101), (N_GRP, GROUPS), 0, 1 << 20) * GROUPS + jnp.arange(GROUPS, dtype=jnp.int32)[None, :]
    group_order = jnp.argsort(group_scores, axis=1).astype(jnp.int32)
    user_scores = jax.random.randint(jax.random.fold_in(key, 202), (N_GRP, GROUPS, USERS), 0, 1 << 20) * USERS + jnp.arange(USERS, dtype=jnp.int32)[None, None, :]
    user_order = jnp.argsort(user_scores, axis=2).astype(jnp.int32)
    member_scores = jax.random.randint(jax.random.fold_in(key, 303), (N_GRP, GROUPS, GROUP_EXP), 0, 1 << 20) * GROUP_EXP + jnp.arange(GROUP_EXP, dtype=jnp.int32)[None, None, :]
    member_order = jnp.argsort(member_scores, axis=2).astype(jnp.int32)
    ticket = TOPG * jnp.arange(ROWS_GRP, dtype=jnp.int32)[:, None] + jnp.arange(TOPG, dtype=jnp.int32)[None, :]
    position = ticket % GROUPS
    cycle_index = ticket // GROUPS
    blocks = jnp.arange(N_GRP, dtype=jnp.int32)[:, None, None]
    group_id = group_order[blocks, position[None, :, :]]
    user_slot = user_order[blocks, position[None, :, :], cycle_index[None, :, :]]
    pick_index = user_slot[:, :, :, None] + USERS * jnp.arange(PICK, dtype=jnp.int32)[None, None, None, :]
    member_rank = jnp.where(pick_index < CAP, 0, 1 + (pick_index - CAP) % (GROUP_EXP - 1))
    member = member_order[blocks[:, :, :, None], position[None, :, :, None], member_rank]
    experts = group_id[:, :, :, None] * GROUP_EXP + member
    return experts.reshape(TOKENS, TOPK).astype(jnp.int32)


def level_of(stream_key, extent, shards, low, top_value):
    loudness = 1.0
    for dim, blocks in shards:
        draws = jax.random.uniform(jax.random.fold_in(jax.random.fold_in(stream_key, 6), dim), (blocks,), jnp.float32, low / len(shards), top_value / len(shards))
        loudness = loudness * jnp.repeat(jnp.exp(draws), extent[dim] // blocks).reshape((-1,) + (1,) * (len(extent) - 1 - dim))
    return loudness


def bell_draw(key, shape, scale, reach, pieces=(), kind=jnp.bfloat16):
    entries = scale * jax.random.normal(key, shape, jnp.float32)
    if pieces:
        entries = entries * level_of(key, shape, pieces, -0.22, 0.18)
    return jnp.clip(entries, -reach, reach).astype(kind)


def setup_inputs(seed: int = 0) -> dict:
    key_list = jax.random.split(jax.random.key(seed), 7)
    return {
        "out_grad": bell_draw(key_list[0], (TOKENS, D), 1.0, 6.0, ((0, 64), (1, 16))),
        "expert_ids": draw_expert_ids(jax.random.fold_in(key_list[6], 71), 0),
        "router_logits": bell_draw(key_list[2], (TOKENS, EXPERTS), 1.0, 5.0, ((0, 64),), jnp.float32),
        "router_weight": bell_draw(key_list[3], (EXPERTS, D), D ** -0.5, 0.09375, ((1, 16),)),
        "expert_weight": bell_draw(key_list[4], (EXPERTS, D, FF), FF ** -0.5, 0.1875, ((0, 64), (1, 16))),
        "hidden_saved": bell_draw(key_list[5], (N_GRP, SLOTS, FF), 1.0, 6.0, ((0, 64),)),
    }


route_scale = 2.5


def slot_places(expert_ids):
    pair_rows = expert_ids.reshape(N_GRP, ROWS_GRP * TOPK)
    onehot = (pair_rows[:, :, None] == jnp.arange(EXPERTS, dtype=jnp.int32)[None, None, :]).astype(jnp.int32)
    pair_ranks = jnp.sum((jnp.cumsum(onehot, axis=1) - 1) * onehot, axis=2)
    source_block = jnp.arange(N_GRP, dtype=jnp.int32)[:, None]
    within = ((pair_rows % EXP_GRP) * N_GRP + source_block) * CAP + pair_ranks
    return ((pair_rows // EXP_GRP) * SLOTS + within).reshape(TOKENS * TOPK).astype(jnp.int32)


def reference(out_grad, expert_ids, router_logits, router_weight, expert_weight, hidden_saved):
    sig = jax.nn.sigmoid(router_logits.astype(jnp.float32))
    chosen = jnp.take_along_axis(sig, expert_ids, axis=1)
    route_probs = route_scale * chosen / jnp.sum(chosen, axis=1, keepdims=True)
    places = slot_places(expert_ids)
    pair_token = (jnp.arange(TOKENS * TOPK, dtype=jnp.int32) // TOPK).astype(jnp.int32)
    token_of_slot = jnp.zeros((N_GRP * SLOTS,), jnp.int32).at[places].set(pair_token)
    used_slot = jnp.zeros((N_GRP * SLOTS,), jnp.int32).at[places].set(jnp.ones((TOKENS * TOPK,), jnp.int32))
    slot_prob = jnp.zeros((N_GRP * SLOTS,), jnp.float32).at[places].set(route_probs.reshape(TOKENS * TOPK)).astype(jnp.bfloat16)
    span = N_GRP * CAP
    width = D // N_EP

    def owner_work(items):
        token_index, used_flag, prob_row, saved_rows, weights = items
        slot_rows = jnp.where(used_flag[:, None] > 0, out_grad[token_index], jnp.zeros((), jnp.bfloat16))
        grouped = slot_rows.reshape(EXP_GRP, span, N_EP, width).astype(jnp.float32)
        split_weights = weights.reshape(EXP_GRP, N_EP, width, FF).astype(jnp.float32)
        partial_sums = jnp.einsum("lmkd,lkdf->lkmf", grouped, split_weights)
        rounded = lax.optimization_barrier(partial_sums.astype(jnp.bfloat16)).astype(jnp.float32)
        summed = jnp.sum(rounded, axis=1).reshape(SLOTS, FF)
        prob_value = prob_row.astype(jnp.float32)
        hidden_grad = (prob_value[:, None] * summed).astype(jnp.bfloat16)
        slot_score = jnp.sum(saved_rows.astype(jnp.float32) * summed, axis=1)
        scaled_rows = (prob_value[:, None] * slot_rows.astype(jnp.float32)).astype(jnp.bfloat16)
        weight_grad = jnp.einsum(
            "lmd,lmf->ldf",
            scaled_rows.reshape(EXP_GRP, span, D).astype(jnp.float32),
            saved_rows.reshape(EXP_GRP, span, FF).astype(jnp.float32),
        ).astype(jnp.bfloat16)
        return weight_grad, hidden_grad, slot_score

    weight_grad, hidden_grad, slot_score = lax.map(
        owner_work,
        (
            token_of_slot.reshape(N_GRP, SLOTS),
            used_slot.reshape(N_GRP, SLOTS),
            slot_prob.reshape(N_GRP, SLOTS),
            hidden_saved,
            expert_weight.reshape(N_GRP, EXP_GRP, D, FF),
        ),
    )
    pair_score = slot_score.reshape(N_GRP * SLOTS)[places].reshape(TOKENS, TOPK)
    weighted_mean = jnp.sum(route_probs * pair_score, axis=1, keepdims=True) / route_scale
    logit_terms = route_probs * (1.0 - chosen) * (pair_score - weighted_mean)
    picked = expert_ids[:, :, None] == jnp.arange(EXPERTS, dtype=jnp.int32)[None, None, :]
    router_grad = jnp.sum(jnp.where(picked, logit_terms[:, :, None], jnp.zeros((), jnp.float32)), axis=1).astype(jnp.bfloat16)
    input_grad = jnp.dot(router_grad, router_weight, preferred_element_type=jnp.float32).astype(jnp.bfloat16)
    return weight_grad.reshape(EXPERTS, D, FF), hidden_grad, input_grad
```

```python
import functools
import jax
import jax.numpy as jnp
from jax import lax
from jax.experimental import pallas as pl
from jax.experimental.pallas import tpu as pltpu
from jax.sharding import PartitionSpec as P

route_scale = 2.5
cap = 16
unset = 255.0
bf16 = jnp.bfloat16
f32 = jnp.float32
MESH = pl.DeviceIdType.MESH


def iota(shape, dim):
    return lax.broadcasted_iota(jnp.int32, shape, dim)


def kernel(n, og_ref, ids_ref, lg_ref, rw_ref, ew_ref, hs_ref, wg_ref, hg_ref, ig_ref,
           hs_v, w_v, wp_v, tok, tk, tbs0, tbs1, tb0, tb1, sb0, sb1, r0, r1, e0, e1,
           dacc, ds, dr, g_v, pb, sr, wg_v, s_v, sa, bs, sc, ct, q_s, q_c, q_y, q_r,
           acc, snd, rcv, code_v, prob_v, sig_v,
           loc_sem, s1_send, s1_recv, s2_send, s2_recv, d_send, d_recv, x_send, x_recv,
           a_send, a_recv, b_send, b_recv, y_send, y_recv, r_send, r_recv):
    tokens, half = og_ref.shape[0], og_ref.shape[1] // 2
    topk = ids_ref.shape[1]
    experts = lg_ref.shape[1]
    width = hs_v.shape[1]
    ge = 2 * n
    hn = n // 2
    ch = n * cap
    rows = hn * cap
    subs = min(2, hn)
    sub = rows // subs
    g = lax.axis_index("grp")
    k = lax.axis_index("ep")
    x, z = g // n, lax.rem(g, n)
    y, c = k // 2, lax.rem(k, 2)
    wrap = lambda v: lax.rem(v + 2 * n, n)
    at_x = lambda v: (v * n + z, k)
    at_z = lambda v: (x * n + v, k)
    at_y = lambda v: (g, v * 2 + c)
    partner = (g, y * 2 + 1 - c)

    def rcopy(src, dst, ss, rs, dev):
        return pltpu.make_async_remote_copy(
            src_ref=src, dst_ref=dst, send_sem=ss, recv_sem=rs, device_id=dev, device_id_type=MESH)

    w_in = pltpu.make_async_copy(ew_ref, w_v, loc_sem.at[0])
    w_in.start()
    hs_in = pltpu.make_async_copy(hs_ref, hs_v, loc_sem.at[1])
    hs_in.start()
    barrier = pltpu.get_barrier_semaphore()
    for d in range(1, n):
        for at, me in ((at_x, x), (at_z, z), (at_y, y)):
            pl.semaphore_signal(barrier, inc=1, device_id=at(wrap(me + d)), device_id_type=MESH)
    pl.semaphore_signal(barrier, inc=1, device_id=partner, device_id_type=MESH)

    ids = ids_ref[...]
    lane_e = iota((tokens, experts), 1)
    member = jnp.zeros((tokens, experts), f32)
    for i in range(topk):
        member += (ids[:, i:i + 1] == lane_e).astype(f32)
    lower = (iota((tokens, tokens), 0) > iota((tokens, tokens), 1)).astype(f32).astype(bf16)
    rank = jnp.dot(lower, member.astype(bf16), preferred_element_type=f32)
    code = jnp.where(member > 0.0, rank, unset)
    sig = jax.nn.sigmoid(lg_ref[...])
    chosen = member * sig
    prob = route_scale * chosen / jnp.sum(chosen, axis=1, keepdims=True)
    code_v[...] = code
    prob_v[...] = prob
    sig_v[...] = sig
    code_t = code.T
    prob_t = prob.T.astype(bf16)
    row_e, col_e = iota((experts, experts), 0), iota((experts, experts), 1)
    perm = (col_e == (row_e // 2 % n) * ge + (row_e // ge) * 2 + row_e % 2).astype(f32).astype(bf16)
    code_t = code_t.astype(bf16)
    code_p = jnp.dot(perm, code_t, preferred_element_type=f32).astype(bf16)
    for v in range(n):
        tbs0[v, 0:ge, :] = code_t[v * ge:(v + 1) * ge, :]
        tbs0[v, ge:2 * ge, :] = prob_t[v * ge:(v + 1) * ge, :]
        tbs1[v] = code_p[v * ge:(v + 1) * ge, :]
    og = og_ref[...]
    tok[0] = og[:, :half]
    tok[1] = og[:, half:]
    tk[0, x] = og[:, :half]
    tk[1, z] = og[:, half:]
    tb0[x] = tbs0[x]
    tb1[z] = tbs1[z]

    pl.semaphore_wait(barrier, 3 * (n - 1) + 1)

    order = [d if i == 0 else n - d for d in range(1, hn + 1) for i in range(2)][: n - 1]

    def tok0(v):
        return rcopy(tok.at[0], tk.at[0, x], s1_send.at[0, v], s1_recv.at[0, x], at_x(v))

    def tok1(v):
        return rcopy(tok.at[1], tk.at[1, z], s1_send.at[1, v], s1_recv.at[1, z], at_z(v))

    def tab0(v):
        return rcopy(tbs0.at[v], tb0.at[x], s1_send.at[2, v], s1_recv.at[2, x], at_x(v))

    def tab1(v):
        return rcopy(tbs1.at[v], tb1.at[z], s1_send.at[3, v], s1_recv.at[3, z], at_z(v))

    for d in order:
        tab0(wrap(x + d)).start()
        tok0(wrap(x + d)).start()
        tab1(wrap(z + d)).start()
        tok1(wrap(z + d)).start()

    w_in.wait()
    w_out = rcopy(w_v, wp_v, x_send.at[0], x_recv.at[0], partner)
    w_out.start()

    slot_r = iota((ge, cap, tokens), 1).astype(f32)
    dacc[...] = jnp.zeros_like(dacc)

    def fill(path, table):
        hot = (table.astype(f32)[:, None, :] == slot_r).astype(f32).astype(bf16)
        hot = hot.reshape(ge * cap, tokens)
        return hot

    def out0(v, us):
        return rcopy(sb0.at[v, us], r0.at[z, us // 2, lax.rem(us, 2)], s2_send.at[0, v], s2_recv.at[0, z], at_z(v))

    def out1(v, us):
        return rcopy(sb1.at[v, us], r1.at[x // 2, lax.rem(x, 2), us], s2_send.at[1, v], s2_recv.at[1, x], at_x(v))

    def spread0(us):
        hot = fill(0, tb0[us, 0:ge, :])
        got = jnp.dot(hot, tk[0, us], preferred_element_type=f32).astype(bf16)
        sb0[:, us] = got.reshape(n, 2, cap, half)
        for d in order:
            out0(wrap(z + d), us).start()
        r0[z, us // 2, lax.rem(us, 2)] = sb0[z, us]
        table = tb0[us, ge:2 * ge, :]
        wide = jnp.concatenate([table] * n, axis=0)
        wide = jnp.where(iota((experts, tokens), 0) // ge == us, wide.astype(f32), 0.0).astype(bf16)
        dacc[...] += lax.dot_general(hot, wide, (((1,), (1,)), ((), ())), preferred_element_type=f32)

    def spread1(us):
        hot = fill(1, tb1[us])
        got = jnp.dot(hot, tk[1, us], preferred_element_type=f32).astype(bf16)
        sb1[:, us] = got.reshape(n, 2, cap, half)
        for d in order:
            out1(wrap(x + d), us).start()
        r1[x // 2, lax.rem(x, 2), us] = sb1[x, us]

    spread0(x)
    spread1(z)

    def arrive(j, carry):
        off = (j + 1) // 2
        off = jnp.where(lax.rem(j, 2) == 1, off, n - off)
        ux, uz = wrap(x + off), wrap(z + off)
        rcopy(tbs0.at[0], tb0.at[ux], s1_send.at[2, 0], s1_recv.at[2, ux], partner).wait_recv()
        rcopy(tok.at[0], tk.at[0, ux], s1_send.at[0, 0], s1_recv.at[0, ux], partner).wait_recv()
        spread0(ux)
        rcopy(tbs1.at[0], tb1.at[uz], s1_send.at[3, 0], s1_recv.at[3, uz], partner).wait_recv()
        rcopy(tok.at[1], tk.at[1, uz], s1_send.at[1, 0], s1_recv.at[1, uz], partner).wait_recv()
        spread1(uz)
        return carry

    lax.fori_loop(1, n, arrive, 0)

    ds[...] = dacc[...].astype(bf16).reshape(n, 2 * cap, experts)
    dr[z] = ds[z]

    def dout(v):
        return rcopy(ds.at[v], dr.at[z], d_send.at[v], d_recv.at[z], at_z(v))

    for d in order:
        dout(wrap(z + d)).start()

    hs_in.wait()
    tile = ch * n // 4

    def gmul(i, carry):
        l = i // 4
        at = pl.multiple_of(i * tile, tile)
        g_v[pl.ds(at, tile), :] = lax.dot_general(
            hs_v[pl.ds(at, tile), :], w_v[l], (((1,), (1,)), ((), ())), preferred_element_type=f32)
        return carry

    lax.fori_loop(0, 8, gmul, 0)

    for d in order:
        vz, vx = wrap(z + d), wrap(x + d)
        rcopy(sb0.at[0], r0.at[vz], s2_send.at[0, 0], s2_recv.at[0, vz], partner).wait_recv()
        rcopy(sb1.at[0], r1.at[vx // 2, lax.rem(vx, 2)], s2_send.at[1, 0], s2_recv.at[1, vx], partner).wait_recv()

    ex0 = rcopy(r0.at[:, :, 1 - c], e0, x_send.at[1], x_recv.at[1], partner)
    ex1 = rcopy(r1.at[:, 1 - c], e1, x_send.at[2], x_recv.at[2], partner)
    ex0.start()
    ex1.start()

    eye = iota((ch, ch), 0) == iota((ch, ch), 1)
    for l in range(2):
        for xb in range(n):
            q = l * n * ch + xb * ch
            a0 = r0[:, xb // 2, xb % 2, l].reshape(ch, half).astype(f32)
            a1 = r1[xb // 2, xb % 2, :, l].reshape(ch, half).astype(f32)
            s = a0 * g_v[q:q + ch, :half] + a1 * g_v[q:q + ch, half:]
            s = jnp.sum(s, axis=1, keepdims=True)
            s_v[l * n + xb:l * n + xb + 1, :] = jnp.sum(jnp.where(eye, s, 0.0), axis=0, keepdims=True)

    w_out.wait_recv()
    ex0.wait_recv()
    ex1.wait_recv()

    def partial(chunk, d):
        l, xh = chunk // hn, lax.rem(chunk, hn)
        zs = pl.ds(d * hn, hn)
        own = jnp.concatenate(
            [r0[zs, xh, c, l].reshape(rows, half), r1[xh, c, zs, l].reshape(rows, half)], axis=1)
        other = jnp.concatenate(
            [e0[zs, xh, l].reshape(rows, half), e1[xh, zs, l].reshape(rows, half)], axis=1)
        step = width // 4
        for j in range(4):
            cols = slice(j * step, (j + 1) * step)
            acc[d, :, cols] = jnp.dot(own, w_v[l, :, cols], preferred_element_type=f32) + jnp.dot(
                other, wp_v[l, :, cols], preferred_element_type=f32)

    def hop(s, d, i):
        to = at_y(wrap(y + 1)) if d == 0 else at_y(wrap(y - 1 + n))
        return rcopy(snd.at[d, s, i], rcv.at[d, s, i], r_send.at[d, s, i], r_recv.at[d, s, i], to)

    def ring(s):
        for d in range(2):
            partial(wrap(y - 1 - s + n) if d == 0 else wrap(y + 1 + s), d)
        for i in range(subs):
            for d in range(2):
                val = acc[d, i * sub:(i + 1) * sub, :]
                if s > 0:
                    hop(s - 1, d, i).wait_recv()
                    val = val + rcv[d, s - 1, i].astype(f32)
                snd[d, s, i] = val.astype(bf16)
                hop(s, d, i).start()

    def aout(v):
        return rcopy(s_v, sa.at[z], a_send.at[v], a_recv.at[z], at_z(v))

    def bout(v):
        return rcopy(bs.at[v], sc.at[x], b_send.at[v], b_recv.at[x], at_x(v))

    def yout(v):
        return rcopy(q_y, q_r.at[y], y_send.at[v], y_recv.at[y], at_y(v))

    qx = rcopy(q_s, q_c, x_send.at[3], x_recv.at[3], partner)

    def score_a():
        sa[z] = s_v[...]
        for d in order:
            aout(wrap(z + d)).start()

    def score_b():
        for d in order:
            v = wrap(z + d)
            rcopy(s_v, sa.at[v], a_send.at[0], a_recv.at[v], partner).wait_recv()
        for v in range(n):
            for l in range(2):
                for xb in range(n):
                    bs[xb, v * 2 + l:v * 2 + l + 1, :] = sa[v, l * n + xb:l * n + xb + 1, :]
        sc[x] = bs[x]
        for d in order:
            bout(wrap(x + d)).start()

    def score_c():
        for d in order:
            v = wrap(x + d)
            rcopy(bs.at[0], sc.at[v], b_send.at[0], b_recv.at[v], partner).wait_recv()
        ct[...] = sc[...].reshape(experts, ch).T
        q_s[...] = ct[pl.ds(pl.multiple_of(z * cap, cap), cap), :]
        qx.start()

    def score_d():
        qx.wait_recv()
        q_y[...] = q_s[...] + q_c[...]
        q_r[y] = q_y[...]
        for d in order:
            yout(wrap(y + d)).start()

    def finish():
        for d in order:
            v = wrap(y + d)
            rcopy(q_y, q_r.at[v], y_send.at[0], y_recv.at[v], partner).wait_recv()
        total = q_r[0]
        for v in range(1, n):
            total = total + q_r[v]
        codes = code_v[...]
        pair = jnp.zeros((tokens, experts), f32)
        for r in range(cap):
            pair += jnp.where(codes == float(r), total[r:r + 1, :], 0.0)
        probs = prob_v[...]
        mean = jnp.sum(probs * pair, axis=1, keepdims=True) / route_scale
        grad = (probs * (1.0 - sig_v[...]) * (pair - mean)).astype(bf16)
        ig_ref[...] = jnp.dot(grad, rw_ref[...], preferred_element_type=f32).astype(bf16)

    def probs_in():
        for d in order:
            v = wrap(z + d)
            rcopy(ds.at[0], dr.at[v], d_send.at[0], d_recv.at[v], partner).wait_recv()
        mine = dr[...].reshape(n * 2 * cap, experts).astype(f32)
        shape = (n * 2 * cap, experts)
        keep = iota(shape, 1) % ge == z * 2 + iota(shape, 0) // cap % 2
        mine = jnp.where(keep, mine, 0.0).astype(bf16)
        wide = (experts, n * half)
        pick = (iota(wide, 0) // ge == iota(wide, 1) // half).astype(f32).astype(bf16)
        pb[...] = jnp.dot(mine, pick, preferred_element_type=f32).reshape(n, 2, cap, n * half)
        for l in range(2):
            for xb in range(n):
                p = pb[:, l, :, xb * half:(xb + 1) * half].reshape(ch, half)
                a0 = r0[:, xb // 2, xb % 2, l].reshape(ch, half).astype(f32)
                a1 = r1[xb // 2, xb % 2, :, l].reshape(ch, half).astype(f32)
                sr[l, xb * ch:(xb + 1) * ch, :half] = (p * a0).astype(bf16)
                sr[l, xb * ch:(xb + 1) * ch, half:] = (p * a1).astype(bf16)

    wg_out = [pltpu.make_async_copy(wg_v.at[l], wg_ref.at[l], loc_sem.at[2 + l]) for l in range(2)]

    def grads(l):
        step = width // 4
        for j in range(4):
            cols = slice(j * step, (j + 1) * step)
            wg_v[l, :, cols] = lax.dot_general(
                sr[l], hs_v[l * n * ch:(l + 1) * n * ch, cols], (((0,), (0,)), ((), ())),
                preferred_element_type=f32).astype(bf16)
        wg_out[l].start()

    extra = {0: score_a, 1: score_b, 2: score_c, 3: score_d, 4: probs_in,
             5: lambda: grads(0), 6: lambda: grads(1)}
    if n < 8:
        todo = list(extra.values())
        extra = {0: lambda: [f() for f in todo]}
    for s in range(n - 1):
        ring(s)
        if s in extra:
            extra[s]()
    for d in range(2):
        partial(y, d)
    mine_l, mine_x = k // n, lax.rem(k, n)
    for i in range(subs):
        for d in range(2):
            hop(n - 2, d, i).wait_recv()
            val = acc[d, i * sub:(i + 1) * sub, :] + rcv[d, n - 2, i].astype(f32)
            zs = pl.ds(d * hn + i * (hn // subs), hn // subs)
            p = pb[zs, mine_l, :, pl.ds(pl.multiple_of(mine_x * half, half), half)].reshape(sub, half)
            for j in range(width // half):
                cols = slice(j * half, (j + 1) * half)
                at = d * rows + i * sub
                hg_ref[at:at + sub, cols] = (p * val[:, cols]).astype(bf16)
    finish()

    w_out.wait_send()
    ex0.wait_send()
    ex1.wait_send()
    qx.wait_send()
    for d in order:
        vx, vz, vy = wrap(x + d), wrap(z + d), wrap(y + d)
        tok0(vx).wait_send()
        tok1(vz).wait_send()
        tab0(vx).wait_send()
        tab1(vz).wait_send()
        rcopy(sb0.at[vz], r0.at[z], s2_send.at[0, vz], s2_recv.at[0, z], partner).wait_send()
        rcopy(sb1.at[vx], r1.at[x // 2, lax.rem(x, 2)], s2_send.at[1, vx], s2_recv.at[1, x], partner).wait_send()
        dout(vz).wait_send()
        aout(vz).wait_send()
        bout(vx).wait_send()
        yout(vy).wait_send()
    for s in range(n - 1):
        for i in range(subs):
            for d in range(2):
                hop(s, d, i).wait_send()
    for l in range(2):
        wg_out[l].wait()


def body(n, out_grad, expert_ids, router_logits, router_weight, expert_weight, hidden_saved):
    tokens, features = out_grad.shape
    half = features // 2
    experts = router_logits.shape[1]
    width = expert_weight.shape[2]
    slots = hidden_saved.shape[1]
    ge, hn, ch = 2 * n, n // 2, n * cap
    rows, subs = hn * cap, min(2, hn)
    vm = pltpu.VMEM
    dma = pltpu.SemaphoreType.DMA
    scratch = [
        vm((slots, width), bf16), vm((2, features, width), bf16), vm((2, features, width), bf16),
        vm((2, tokens, half), bf16), vm((2, n, tokens, half), bf16),
        vm((n, 2 * ge, tokens), bf16), vm((n, ge, tokens), bf16),
        vm((n, 2 * ge, tokens), bf16), vm((n, ge, tokens), bf16),
        vm((n, n, 2, cap, half), bf16), vm((n, n, 2, cap, half), bf16),
        vm((n, hn, 2, 2, cap, half), bf16), vm((hn, 2, n, 2, cap, half), bf16),
        vm((n, hn, 2, cap, half), bf16), vm((hn, n, 2, cap, half), bf16),
        vm((ge * cap, experts), f32), vm((n, 2 * cap, experts), bf16), vm((n, 2 * cap, experts), bf16),
        vm((slots, features), f32), vm((n, 2, cap, n * half), f32), vm((2, n * ch, features), bf16),
        vm((2, features, width), bf16),
        vm((ge, ch), f32), vm((n, ge, ch), f32), vm((n, ge, ch), f32), vm((n, ge, ch), f32),
        vm((ch, experts), f32),
        vm((cap, experts), f32), vm((cap, experts), f32), vm((cap, experts), f32), vm((n, cap, experts), f32),
        vm((2, rows, width), f32), vm((2, n - 1, subs, rows // subs, width), bf16),
        vm((2, n - 1, subs, rows // subs, width), bf16),
        vm((tokens, experts), f32), vm((tokens, experts), f32), vm((tokens, experts), f32),
        dma((4,)), dma((4, n)), dma((4, n)), dma((2, n)), dma((2, n)), dma((n,)), dma((n,)),
        dma((4,)), dma((4,)), dma((n,)), dma((n,)), dma((n,)), dma((n,)), dma((n,)), dma((n,)),
        dma((2, n - 1, subs)), dma((2, n - 1, subs)),
    ]
    in_vmem = pl.BlockSpec(memory_space=pltpu.VMEM)
    in_hbm = pl.BlockSpec(memory_space=pltpu.HBM)
    weight_grad, hidden_grad, input_grad = pl.pallas_call(
        functools.partial(kernel, n),
        out_shape=(
            jax.ShapeDtypeStruct((2, features, width), bf16),
            jax.ShapeDtypeStruct((ch, width), bf16),
            jax.ShapeDtypeStruct((tokens, features), bf16),
        ),
        in_specs=[in_vmem, in_vmem, in_vmem, in_vmem, in_hbm, in_hbm],
        out_specs=(in_hbm, in_vmem, in_vmem),
        scratch_shapes=scratch,
        compiler_params=pltpu.CompilerParams(collective_id=0, has_side_effects=True),
    )(out_grad, expert_ids, router_logits, router_weight, expert_weight, hidden_saved.reshape(slots, width))
    return weight_grad, hidden_grad[None], input_grad


def solution(mesh):
    n = mesh.shape["ep"] // 2
    in_specs = (
        P("grp", "ep"),
        P("grp", None),
        P("grp", None),
        P(None, "ep"),
        P("grp", "ep", None),
        P("grp", None, None),
    )
    out_specs = (P("grp", "ep", None), P("grp", "ep", None), P("grp", "ep"))
    return jax.shard_map(functools.partial(body, n), mesh=mesh, in_specs=in_specs, out_specs=out_specs, check_vma=False)
```

```python
import functools
import jax
import jax.numpy as jnp
from jax import lax
from jax.experimental import pallas as pl
from jax.experimental.pallas import tpu as pltpu
from jax.sharding import PartitionSpec as P

route_scale = 2.5
cap = 16
unset = 255.0
bf16 = jnp.bfloat16
f32 = jnp.float32
MESH = pl.DeviceIdType.MESH


def iota(shape, dim):
    return lax.broadcasted_iota(jnp.int32, shape, dim)


def kernel(n, og_ref, ids_ref, lg_ref, rw_ref, ew_ref, hs_ref, wg_ref, hg_ref, ig_ref,
           ids_v, lg_v, rw_v, hs_v, w_v, wp_v, tok, tk, tbs0, tbs1, tb0, tb1, sb0, sb1, r0, r1, e0, e1,
           dacc, ds, dr, g_v, pb, sr, s_v, sa, bs, sc, ct, q_s, q_c, q_y, q_r,
           acc, snd, rcv, code_v, prob_v,
           loc_sem, t_send, s1_send, s1_recv, s2_send, s2_recv, d_send, d_recv, x_send, x_recv,
           a_send, a_recv, b_send, b_recv, y_send, y_recv, r_send, r_recv):
    tokens, half = og_ref.shape[0], og_ref.shape[1] // 2
    topk = ids_ref.shape[0]
    experts = lg_ref.shape[1]
    width = hs_v.shape[1]
    ge = 2 * n
    hn = n // 2
    ch = n * cap
    rows = hn * cap
    parts = 2
    wide_part = width // parts
    g = lax.axis_index("grp")
    k = lax.axis_index("ep")
    x, z = g // n, lax.rem(g, n)
    y, c = k // 2, lax.rem(k, 2)
    wrap = lambda v: lax.rem(v + 2 * n, n)
    at_x = lambda v: (v * n + z, k)
    at_z = lambda v: (x * n + v, k)
    at_y = lambda v: (g, v * 2 + c)
    partner = (g, y * 2 + 1 - c)

    def rcopy(src, dst, ss, rs, dev):
        return pltpu.make_async_remote_copy(
            src_ref=src, dst_ref=dst, send_sem=ss, recv_sem=rs, device_id=dev, device_id_type=MESH)

    barrier = pltpu.get_barrier_semaphore()
    for d in range(1, n):
        for at, me in ((at_x, x), (at_z, z), (at_y, y)):
            pl.semaphore_signal(barrier, inc=1, device_id=at(wrap(me + d)), device_id_type=MESH)
    pl.semaphore_signal(barrier, inc=1, device_id=partner, device_id_type=MESH)

    def local(src, dst, i):
        copy = pltpu.make_async_copy(src, dst, loc_sem.at[i])
        copy.start()
        return copy

    ids_in = local(ids_ref, ids_v, 0)
    lg_in = local(lg_ref, lg_v, 1)
    tok_in = [local(og_ref.at[:, p * half:(p + 1) * half], tok.at[p], 2 + p) for p in range(2)]
    w_in = local(ew_ref, w_v, 4)
    hs_in = local(hs_ref, hs_v, 5)
    rw_in = local(rw_ref, rw_v, 6)

    for p in range(2):
        tok_in[p].wait()
    pl.semaphore_wait(barrier, 3 * (n - 1) + 1)

    order = [d if i == 0 else n - d for d in range(1, hn + 1) for i in range(2)][: n - 1]

    def tok0(v):
        return rcopy(tok.at[0], tk.at[0, x], t_send.at[0, v], s1_recv.at[0, x], at_x(v))

    def tok1(v):
        return rcopy(tok.at[1], tk.at[1, z], t_send.at[1, v], s1_recv.at[1, z], at_z(v))

    for d in order:
        tok0(wrap(x + d)).start()
        tok1(wrap(z + d)).start()
    tk[0, x] = tok[0]
    tk[1, z] = tok[1]

    ids_in.wait()
    row_t = iota((experts, tokens), 0)
    member = jnp.zeros((experts, tokens), f32)
    for i in range(topk):
        member += (ids_v[i:i + 1, :] == row_t).astype(f32)
    upper = (iota((tokens, tokens), 0) < iota((tokens, tokens), 1)).astype(f32).astype(bf16)
    rank = jnp.dot(member.astype(bf16), upper, preferred_element_type=f32)
    code = jnp.where(member > 0.0, rank, unset)
    code_v[...] = code
    code_t = code.astype(bf16)
    row_e, col_e = iota((experts, experts), 0), iota((experts, experts), 1)
    perm = (col_e == (row_e // 2 % n) * ge + (row_e // ge) * 2 + row_e % 2).astype(f32).astype(bf16)
    code_p = jnp.dot(perm, code_t, preferred_element_type=f32).astype(bf16)
    lg_in.wait()
    chosen = member * jax.nn.sigmoid(lg_v[...].T)
    prob = route_scale * chosen / jnp.sum(chosen, axis=0, keepdims=True)
    prob_v[...] = prob
    prob_t = prob.astype(bf16)
    for v in range(n):
        tbs0[v, 0:ge, :] = code_t[v * ge:(v + 1) * ge, :]
        tbs0[v, ge:2 * ge, :] = prob_t[v * ge:(v + 1) * ge, :]
        tbs1[v] = code_p[v * ge:(v + 1) * ge, :]
    tb0[x] = tbs0[x]
    tb1[z] = tbs1[z]

    def tab0(v):
        return rcopy(tbs0.at[v], tb0.at[x], s1_send.at[0, v], s1_recv.at[2, x], at_x(v))

    def tab1(v):
        return rcopy(tbs1.at[v], tb1.at[z], s1_send.at[1, v], s1_recv.at[3, z], at_z(v))

    for d in order:
        tab0(wrap(x + d)).start()
        tab1(wrap(z + d)).start()

    slot_r = iota((ge, cap, tokens), 1).astype(f32)
    dacc[...] = jnp.zeros_like(dacc)

    def fill(path, table):
        hot = (table.astype(f32)[:, None, :] == slot_r).astype(f32).astype(bf16)
        hot = hot.reshape(ge * cap, tokens)
        return hot

    def out0(v, us):
        return rcopy(sb0.at[v, us], r0.at[z, us // 2, lax.rem(us, 2)], s2_send.at[0, v], s2_recv.at[0, z], at_z(v))

    def out1(v, us):
        return rcopy(sb1.at[v, us], r1.at[x // 2, lax.rem(x, 2), us], s2_send.at[1, v], s2_recv.at[1, x], at_x(v))

    def spread0(us):
        hot = fill(0, tb0[us, 0:ge, :])
        got = jnp.dot(hot, tk[0, us], preferred_element_type=f32).astype(bf16)
        sb0[:, us] = got.reshape(n, 2, cap, half)
        for d in order:
            out0(wrap(z + d), us).start()
        r0[z, us // 2, lax.rem(us, 2)] = sb0[z, us]
        table = tb0[us, ge:2 * ge, :]
        wide = jnp.concatenate([table] * n, axis=0)
        wide = jnp.where(iota((experts, tokens), 0) // ge == us, wide.astype(f32), 0.0).astype(bf16)
        dacc[...] += lax.dot_general(hot, wide, (((1,), (1,)), ((), ())), preferred_element_type=f32)

    def spread1(us):
        hot = fill(1, tb1[us])
        got = jnp.dot(hot, tk[1, us], preferred_element_type=f32).astype(bf16)
        sb1[:, us] = got.reshape(n, 2, cap, half)
        for d in order:
            out1(wrap(x + d), us).start()
        r1[x // 2, lax.rem(x, 2), us] = sb1[x, us]

    spread0(x)
    spread1(z)

    def arrive(j, carry):
        odd = lax.rem(j, 2)
        off = (j + 1) // 2
        off = odd * off + (1 - odd) * (n - off)
        ux, uz = wrap(x + off), wrap(z + off)
        rcopy(tok.at[0], tk.at[0, ux], t_send.at[0, 0], s1_recv.at[0, ux], partner).wait_recv()
        rcopy(tbs0.at[0], tb0.at[ux], s1_send.at[0, 0], s1_recv.at[2, ux], partner).wait_recv()
        spread0(ux)
        rcopy(tok.at[1], tk.at[1, uz], t_send.at[1, 0], s1_recv.at[1, uz], partner).wait_recv()
        rcopy(tbs1.at[0], tb1.at[uz], s1_send.at[1, 0], s1_recv.at[3, uz], partner).wait_recv()
        spread1(uz)
        return carry

    lax.fori_loop(1, n, arrive, 0)

    ds[...] = dacc[...].astype(bf16).reshape(n, 2 * cap, experts)
    dr[z] = ds[z]

    def dout(v):
        return rcopy(ds.at[v], dr.at[z], d_send.at[v], d_recv.at[z], at_z(v))

    for d in order:
        dout(wrap(z + d)).start()

    w_in.wait()
    w_out = rcopy(w_v, wp_v, x_send.at[0], x_recv.at[0], partner)
    w_out.start()

    hs_in.wait()
    tile = ch * n // 4

    def gmul(i, carry):
        l = i // 4
        at = pl.multiple_of(i * tile, tile)
        g_v[pl.ds(at, tile), :] = lax.dot_general(
            hs_v[pl.ds(at, tile), :], w_v[l], (((1,), (1,)), ((), ())), preferred_element_type=f32)
        return carry

    lax.fori_loop(0, 8, gmul, 0)

    ex0 = rcopy(r0.at[:, :, 1 - c], e0, x_send.at[1], x_recv.at[1], partner)
    ex1 = rcopy(r1.at[:, 1 - c], e1, x_send.at[2], x_recv.at[2], partner)

    def give0(v):
        rcopy(r0.at[v, :, 1 - c], e0.at[v], x_send.at[1], x_recv.at[1], partner).start()

    give0(z)
    for d in order:
        vx = wrap(x + d)
        rcopy(sb1.at[0], r1.at[vx // 2, lax.rem(vx, 2)], s2_send.at[1, 0], s2_recv.at[1, vx], partner).wait_recv()
    ex1.start()
    for d in order:
        vz = wrap(z + d)
        rcopy(sb0.at[0], r0.at[vz], s2_send.at[0, 0], s2_recv.at[0, vz], partner).wait_recv()
        give0(vz)

    def scores():
        eye = iota((ch, ch), 0) == iota((ch, ch), 1)
        for l in range(2):
            for xb in range(n):
                q = l * n * ch + xb * ch
                a0 = r0[:, xb // 2, xb % 2, l].reshape(ch, half).astype(f32)
                a1 = r1[xb // 2, xb % 2, :, l].reshape(ch, half).astype(f32)
                s = a0 * g_v[q:q + ch, :half] + a1 * g_v[q:q + ch, half:]
                s = jnp.sum(s, axis=1, keepdims=True)
                s_v[l * n + xb:l * n + xb + 1, :] = jnp.sum(jnp.where(eye, s, 0.0), axis=0, keepdims=True)

    def partial(chunk, d, own, other):
        l, xh = chunk // hn, lax.rem(chunk, hn)
        zs = pl.ds(d * hn, hn)
        if own:
            mine = jnp.concatenate(
                [r0[zs, xh, c, l].reshape(rows, half), r1[xh, c, zs, l].reshape(rows, half)], axis=1)
        if other:
            their = jnp.concatenate(
                [e0[zs, xh, l].reshape(rows, half), e1[xh, zs, l].reshape(rows, half)], axis=1)
        step = width // 4
        for j in range(4):
            cols = slice(j * step, (j + 1) * step)
            total = jnp.dot(mine, w_v[l, :, cols], preferred_element_type=f32) if own else acc[d, :, cols]
            if other:
                total = total + jnp.dot(their, wp_v[l, :, cols], preferred_element_type=f32)
            acc[d, :, cols] = total

    def hop(s, d, i, j):
        to = at_y(wrap(y + 1)) if d == 0 else at_y(wrap(y - 1 + n))
        return rcopy(snd.at[d, s, i, j], rcv.at[d, s, i, j], r_send.at[d, s, i, j], r_recv.at[d, s, i, j], to)

    def at_step(s, d):
        return wrap(y - 1 - s + n) if d == 0 else wrap(y + 1 + s)

    def ring(s):
        if s == 0:
            for d in range(2):
                partial(at_step(0, d), d, True, False)
            score_a()
            w_out.wait_recv()
            ex1.wait_recv()
            ex0.wait_recv()
            for d in range(2):
                partial(at_step(0, d), d, False, True)
        else:
            for d in range(2):
                partial(at_step(s, d), d, True, True)
        for i in range(hn):
            for j in range(parts):
                for d in range(2):
                    val = acc[d, i * cap:(i + 1) * cap, j * wide_part:(j + 1) * wide_part]
                    if s > 0:
                        hop(s - 1, d, i, j).wait_recv()
                        val = val + rcv[d, s - 1, i, j].astype(f32)
                    snd[d, s, i, j] = val.astype(bf16)
                    hop(s, d, i, j).start()

    def aout(v):
        return rcopy(s_v, sa.at[z], a_send.at[v], a_recv.at[z], at_z(v))

    def bout(v):
        return rcopy(bs.at[v], sc.at[x], b_send.at[v], b_recv.at[x], at_x(v))

    def yout(v):
        return rcopy(q_y, q_r.at[y], y_send.at[v], y_recv.at[y], at_y(v))

    qx = rcopy(q_s, q_c, x_send.at[3], x_recv.at[3], partner)

    def score_a():
        scores()
        sa[z] = s_v[...]
        for d in order:
            aout(wrap(z + d)).start()

    def score_b():
        for d in order:
            v = wrap(z + d)
            rcopy(s_v, sa.at[v], a_send.at[0], a_recv.at[v], partner).wait_recv()
        for v in range(n):
            for l in range(2):
                for xb in range(n):
                    bs[xb, v * 2 + l:v * 2 + l + 1, :] = sa[v, l * n + xb:l * n + xb + 1, :]
        sc[x] = bs[x]
        for d in order:
            bout(wrap(x + d)).start()

    def score_c():
        for d in order:
            v = wrap(x + d)
            rcopy(bs.at[0], sc.at[v], b_send.at[0], b_recv.at[v], partner).wait_recv()
        ct[...] = sc[...].reshape(experts, ch).T
        q_s[...] = ct[pl.ds(pl.multiple_of(z * cap, cap), cap), :]
        qx.start()

    def score_d():
        qx.wait_recv()
        q_y[...] = q_s[...] + q_c[...]
        q_r[y] = q_y[...]
        for d in order:
            yout(wrap(y + d)).start()

    def finish():
        rw_in.wait()
        for d in order:
            v = wrap(y + d)
            rcopy(q_y, q_r.at[v], y_send.at[0], y_recv.at[v], partner).wait_recv()
        total = q_r[0]
        for v in range(1, n):
            total = total + q_r[v]
        codes = code_v[...].T
        pair = jnp.zeros((tokens, experts), f32)
        for r in range(cap):
            pair += jnp.where(codes == float(r), total[r:r + 1, :], 0.0)
        probs = prob_v[...].T
        mean = jnp.sum(probs * pair, axis=1, keepdims=True) / route_scale
        grad = (probs * (1.0 - jax.nn.sigmoid(lg_v[...])) * (pair - mean)).astype(bf16)
        ig_ref[...] = jnp.dot(grad, rw_v[...], preferred_element_type=f32).astype(bf16)

    def probs_in():
        for d in order:
            v = wrap(z + d)
            rcopy(ds.at[0], dr.at[v], d_send.at[0], d_recv.at[v], partner).wait_recv()
        mine = dr[...].reshape(n * 2 * cap, experts).astype(f32)
        shape = (n * 2 * cap, experts)
        keep = iota(shape, 1) % ge == z * 2 + iota(shape, 0) // cap % 2
        mine = jnp.where(keep, mine, 0.0).astype(bf16)
        wide = (experts, n * half)
        pick = (iota(wide, 0) // ge == iota(wide, 1) // half).astype(f32).astype(bf16)
        pb[...] = jnp.dot(mine, pick, preferred_element_type=f32).reshape(n, 2, cap, n * half)

    def scale(l):
        for xb in range(n):
            p = pb[:, l, :, xb * half:(xb + 1) * half].reshape(ch, half)
            a0 = r0[:, xb // 2, xb % 2, l].reshape(ch, half).astype(f32)
            a1 = r1[xb // 2, xb % 2, :, l].reshape(ch, half).astype(f32)
            sr[l, xb * ch:(xb + 1) * ch, :half] = (p * a0).astype(bf16)
            sr[l, xb * ch:(xb + 1) * ch, half:] = (p * a1).astype(bf16)

    def grads(i):
        l, j = i // 4, i % 4
        step = width // 4
        cols = slice(j * step, (j + 1) * step)
        wg_ref[l, :, cols] = lax.dot_general(
            sr[l], hs_v[l * n * ch:(l + 1) * n * ch, cols], (((0,), (0,)), ((), ())),
            preferred_element_type=f32).astype(bf16)

    some = lambda f, *items: [functools.partial(f, i) for i in items]
    todo = [[probs_in], [score_b] + some(scale, 0), some(grads, 0, 1), [score_c] + some(scale, 1),
            [score_d] + some(grads, 2, 3), some(grads, 4, 5), some(grads, 6, 7) + [finish]]
    if n < 8:
        todo = [sum(todo, [])]
    for s in range(n - 1):
        ring(s)
        for work in todo[s]:
            work()
    for d in range(2):
        partial(y, d, True, True)
    mine_l, mine_x = k // n, lax.rem(k, n)
    for i in range(hn):
        for j in range(parts):
            for d in range(2):
                hop(n - 2, d, i, j).wait_recv()
                zb = d * hn + i
                p = pb[zb, mine_l, :, pl.ds(pl.multiple_of(mine_x * half, half), half)]
                for m in range(wide_part // half):
                    a, b = j * wide_part + m * half, j * wide_part + (m + 1) * half
                    val = acc[d, i * cap:(i + 1) * cap, a:b]
                    val = val + rcv[d, n - 2, i, j, :, m * half:(m + 1) * half].astype(f32)
                    hg_ref[zb * cap:(zb + 1) * cap, a:b] = (p * val).astype(bf16)

    w_out.wait_send()
    ex0.wait_send()
    ex1.wait_send()
    qx.wait_send()
    for d in order:
        vx, vz, vy = wrap(x + d), wrap(z + d), wrap(y + d)
        tok0(vx).wait_send()
        tok1(vz).wait_send()
        tab0(vx).wait_send()
        tab1(vz).wait_send()
        rcopy(sb0.at[vz], r0.at[z], s2_send.at[0, vz], s2_recv.at[0, z], partner).wait_send()
        rcopy(sb1.at[vx], r1.at[x // 2, lax.rem(x, 2)], s2_send.at[1, vx], s2_recv.at[1, x], partner).wait_send()
        dout(vz).wait_send()
        aout(vz).wait_send()
        bout(vx).wait_send()
        yout(vy).wait_send()
    for s in range(n - 1):
        for i in range(hn):
            for j in range(parts):
                for d in range(2):
                    hop(s, d, i, j).wait_send()


def put_out(wg_ref, hg_ref, ig_ref, wg_out, hg_out, ig_out, sem):
    copies = [
        pltpu.make_async_copy(src, dst, sem.at[i])
        for i, (src, dst) in enumerate(((wg_ref, wg_out), (hg_ref, hg_out), (ig_ref, ig_out)))
    ]
    for copy in copies:
        copy.start()
    for copy in copies:
        copy.wait()


def body(n, out_grad, expert_ids, router_logits, router_weight, expert_weight, hidden_saved):
    tokens, features = out_grad.shape
    half = features // 2
    experts = router_logits.shape[1]
    width = expert_weight.shape[2]
    slots = hidden_saved.shape[1]
    ge, hn, ch = 2 * n, n // 2, n * cap
    rows, parts = hn * cap, 2
    vm = pltpu.VMEM
    dma = pltpu.SemaphoreType.DMA
    scratch = [
        vm(expert_ids.shape[::-1], jnp.int32), vm((tokens, experts), f32), vm((experts, features), bf16),
        vm((slots, width), bf16), vm((2, features, width), bf16), vm((2, features, width), bf16),
        vm((2, tokens, half), bf16), vm((2, n, tokens, half), bf16),
        vm((n, 2 * ge, tokens), bf16), vm((n, ge, tokens), bf16),
        vm((n, 2 * ge, tokens), bf16), vm((n, ge, tokens), bf16),
        vm((n, n, 2, cap, half), bf16), vm((n, n, 2, cap, half), bf16),
        vm((n, hn, 2, 2, cap, half), bf16), vm((hn, 2, n, 2, cap, half), bf16),
        vm((n, hn, 2, cap, half), bf16), vm((hn, n, 2, cap, half), bf16),
        vm((ge * cap, experts), f32), vm((n, 2 * cap, experts), bf16), vm((n, 2 * cap, experts), bf16),
        vm((slots, features), f32), vm((n, 2, cap, n * half), f32), vm((2, n * ch, features), bf16),
        vm((ge, ch), f32), vm((n, ge, ch), f32), vm((n, ge, ch), f32), vm((n, ge, ch), f32),
        vm((ch, experts), f32),
        vm((cap, experts), f32), vm((cap, experts), f32), vm((cap, experts), f32), vm((n, cap, experts), f32),
        vm((2, rows, width), f32), vm((2, n - 1, hn, parts, cap, width // parts), bf16),
        vm((2, n - 1, hn, parts, cap, width // parts), bf16),
        vm((experts, tokens), f32), vm((experts, tokens), f32),
        dma((7,)), dma((2, n)), dma((2, n)), dma((4, n)), dma((2, n)), dma((2, n)), dma((n,)), dma((n,)),
        dma((4,)), dma((4,)), dma((n,)), dma((n,)), dma((n,)), dma((n,)), dma((n,)), dma((n,)),
        dma((2, n - 1, hn, parts)), dma((2, n - 1, hn, parts)),
    ]
    in_vmem = pl.BlockSpec(memory_space=pltpu.VMEM)
    in_hbm = pl.BlockSpec(memory_space=pltpu.HBM)
    weight_grad, hidden_grad, input_grad = pl.pallas_call(
        functools.partial(kernel, n),
        out_shape=(
            pltpu.VMEM((2, features, width), bf16),
            pltpu.VMEM((ch, width), bf16),
            pltpu.VMEM((tokens, features), bf16),
        ),
        in_specs=[in_hbm] * 6,
        out_specs=(in_vmem, in_vmem, in_vmem),
        scratch_shapes=scratch,
        compiler_params=pltpu.CompilerParams(collective_id=0, has_side_effects=True),
    )(out_grad, expert_ids.T, router_logits, router_weight, expert_weight, hidden_saved.reshape(slots, width))
    weight_grad, hidden_grad, input_grad = pl.pallas_call(
        put_out,
        out_shape=(
            jax.ShapeDtypeStruct((2, features, width), bf16),
            jax.ShapeDtypeStruct((ch, width), bf16),
            jax.ShapeDtypeStruct((tokens, features), bf16),
        ),
        in_specs=[pl.BlockSpec(memory_space=pl.ANY)] * 3,
        out_specs=(in_hbm, in_hbm, in_hbm),
        scratch_shapes=[dma((3,))],
        compiler_params=pltpu.CompilerParams(vmem_limit_bytes=1 << 20),
    )(weight_grad, hidden_grad, input_grad)
    return weight_grad, hidden_grad[None], input_grad


def solution(mesh):
    n = mesh.shape["ep"] // 2
    in_specs = (
        P("grp", "ep"),
        P("grp", None),
        P("grp", None),
        P(None, "ep"),
        P("grp", "ep", None),
        P("grp", None, None),
    )
    out_specs = (P("grp", "ep", None), P("grp", "ep", None), P("grp", "ep"))
    return jax.shard_map(functools.partial(body, n), mesh=mesh, in_specs=in_specs, out_specs=out_specs, check_vma=False)
```

```python
import functools
import jax
import jax.numpy as jnp
from jax import lax
from jax.experimental import pallas as pl
from jax.experimental.pallas import tpu as pltpu
from jax.sharding import PartitionSpec as P

route_scale = 2.5
cap = 16
unset = 255.0
bf16 = jnp.bfloat16
f32 = jnp.float32
MESH = pl.DeviceIdType.MESH


def iota(shape, dim):
    return lax.broadcasted_iota(jnp.int32, shape, dim)


def kernel(n, og_ref, ids_ref, lg_ref, rw_ref, ew_ref, hs_ref, wg_ref, hg_ref, ig_ref,
           ids_v, lg_v, rw_v, hs_v, w_v, wp_v, tok, tk, tbs0, tbs1, tb0, tb1, sb0, sb1, r0, r1, e0, e1,
           dacc, ds, dr, g_v, pb, sr, s_v, sa, bs, sc, ct, q_s, q_c, q_y, q_r,
           acc, snd, rcv, code_v, prob_v,
           loc_sem, t_send, s1_send, s1_recv, s2_send, s2_recv, d_send, d_recv, x_send, x_recv,
           a_send, a_recv, b_send, b_recv, y_send, y_recv, r_send, r_recv):
    tokens, half = og_ref.shape[0], og_ref.shape[1] // 2
    topk = ids_ref.shape[0]
    experts = lg_ref.shape[1]
    width = hs_v.shape[1]
    ge = 2 * n
    hn = n // 2
    ch = n * cap
    rows = hn * cap
    parts = 2
    wide_part = width // parts
    g = lax.axis_index("grp")
    k = lax.axis_index("ep")
    x, z = g // n, lax.rem(g, n)
    y, c = k // 2, lax.rem(k, 2)
    wrap = lambda v: lax.rem(v + 2 * n, n)
    at_x = lambda v: (v * n + z, k)
    at_z = lambda v: (x * n + v, k)
    at_y = lambda v: (g, v * 2 + c)
    partner = (g, y * 2 + 1 - c)

    def rcopy(src, dst, ss, rs, dev):
        return pltpu.make_async_remote_copy(
            src_ref=src, dst_ref=dst, send_sem=ss, recv_sem=rs, device_id=dev, device_id_type=MESH)

    barrier = pltpu.get_barrier_semaphore()
    for d in range(1, n):
        for at, me in ((at_x, x), (at_z, z), (at_y, y)):
            pl.semaphore_signal(barrier, inc=1, device_id=at(wrap(me + d)), device_id_type=MESH)
    pl.semaphore_signal(barrier, inc=1, device_id=partner, device_id_type=MESH)

    def local(src, dst, i):
        copy = pltpu.make_async_copy(src, dst, loc_sem.at[i])
        copy.start()
        return copy

    ids_in = local(ids_ref, ids_v, 0)
    lg_in = local(lg_ref, lg_v, 1)
    tok_in = [local(og_ref.at[:, p * half:(p + 1) * half], tok.at[p], 2 + p) for p in range(2)]
    w_in = local(ew_ref, w_v, 4)
    hs_in = local(hs_ref, hs_v, 5)
    rw_in = local(rw_ref, rw_v, 6)

    for p in range(2):
        tok_in[p].wait()
    pl.semaphore_wait(barrier, 3 * (n - 1) + 1)

    order = [d if i == 0 else n - d for d in range(1, hn + 1) for i in range(2)][: n - 1]

    def tok0(v):
        return rcopy(tok.at[0], tk.at[0, x], t_send.at[0, v], s1_recv.at[0, x], at_x(v))

    def tok1(v):
        return rcopy(tok.at[1], tk.at[1, z], t_send.at[1, v], s1_recv.at[1, z], at_z(v))

    near = order[:4]
    for d in near:
        tok0(wrap(x + d)).start()
        tok1(wrap(z + d)).start()
    tk[0, x] = tok[0]
    tk[1, z] = tok[1]

    ids_in.wait()
    row_t = iota((experts, tokens), 0)
    member = jnp.zeros((experts, tokens), f32)
    for i in range(topk):
        member += (ids_v[i:i + 1, :] == row_t).astype(f32)
    upper = (iota((tokens, tokens), 0) < iota((tokens, tokens), 1)).astype(f32).astype(bf16)
    rank = jnp.dot(member.astype(bf16), upper, preferred_element_type=f32)
    code = jnp.where(member > 0.0, rank, unset)
    code_v[...] = code
    code_t = code.astype(bf16)
    row_e, col_e = iota((experts, experts), 0), iota((experts, experts), 1)
    perm = (col_e == (row_e // 2 % n) * ge + (row_e // ge) * 2 + row_e % 2).astype(f32).astype(bf16)
    code_p = jnp.dot(perm, code_t, preferred_element_type=f32).astype(bf16)
    lg_in.wait()
    chosen = member * jax.nn.sigmoid(lg_v[...].T)
    prob = route_scale * chosen / jnp.sum(chosen, axis=0, keepdims=True)
    prob_v[...] = prob
    prob_t = prob.astype(bf16)
    for v in range(n):
        tbs0[v, 0:ge, :] = code_t[v * ge:(v + 1) * ge, :]
        tbs0[v, ge:2 * ge, :] = prob_t[v * ge:(v + 1) * ge, :]
        tbs1[v] = code_p[v * ge:(v + 1) * ge, :]
    tb0[x] = tbs0[x]
    tb1[z] = tbs1[z]

    relays = [(2, -1, 3), (2, -2, 4), (n - 2, 1, 5)] if n > 4 else []

    def far0(off, d, i):
        u = wrap(x + off)
        return rcopy(tk.at[0, u], tk.at[0, u], t_send.at[0, wrap(x + i)], s1_recv.at[0, u], at_x(wrap(x + d)))

    def far1(off, d, i):
        u = wrap(z + off)
        return rcopy(tk.at[1, u], tk.at[1, u], t_send.at[1, wrap(z + i)], s1_recv.at[1, u], at_z(wrap(z + d)))

    def rows_in(ux, uz):
        rcopy(tok.at[0], tk.at[0, ux], t_send.at[0, 0], s1_recv.at[0, ux], partner).wait_recv()
        rcopy(tok.at[1], tk.at[1, uz], t_send.at[1, 0], s1_recv.at[1, uz], partner).wait_recv()

    def tab0(v):
        return rcopy(tbs0.at[v], tb0.at[x], s1_send.at[0, v], s1_recv.at[2, x], at_x(v))

    def tab1(v):
        return rcopy(tbs1.at[v], tb1.at[z], s1_send.at[1, v], s1_recv.at[3, z], at_z(v))

    for d in order:
        tab0(wrap(x + d)).start()
        tab1(wrap(z + d)).start()

    slot_r = iota((ge, cap, tokens), 1).astype(f32)
    dacc[...] = jnp.zeros_like(dacc)

    def fill(path, table):
        hot = (table.astype(f32)[:, None, :] == slot_r).astype(f32).astype(bf16)
        hot = hot.reshape(ge * cap, tokens)
        return hot

    def out0(v, us):
        return rcopy(sb0.at[v, us], r0.at[z, us // 2, lax.rem(us, 2)], s2_send.at[0, v], s2_recv.at[0, z], at_z(v))

    def out1(v, us):
        return rcopy(sb1.at[v, us], r1.at[x // 2, lax.rem(x, 2), us], s2_send.at[1, v], s2_recv.at[1, x], at_x(v))

    def spread0(us):
        hot = fill(0, tb0[us, 0:ge, :])
        got = jnp.dot(hot, tk[0, us], preferred_element_type=f32).astype(bf16)
        sb0[:, us] = got.reshape(n, 2, cap, half)
        for d in order:
            out0(wrap(z + d), us).start()
        r0[z, us // 2, lax.rem(us, 2)] = sb0[z, us]
        table = tb0[us, ge:2 * ge, :]
        wide = jnp.concatenate([table] * n, axis=0)
        wide = jnp.where(iota((experts, tokens), 0) // ge == us, wide.astype(f32), 0.0).astype(bf16)
        dacc[...] += lax.dot_general(hot, wide, (((1,), (1,)), ((), ())), preferred_element_type=f32)

    def spread1(us):
        hot = fill(1, tb1[us])
        got = jnp.dot(hot, tk[1, us], preferred_element_type=f32).astype(bf16)
        sb1[:, us] = got.reshape(n, 2, cap, half)
        for d in order:
            out1(wrap(x + d), us).start()
        r1[x // 2, lax.rem(x, 2), us] = sb1[x, us]

    spread0(x)
    spread1(z)
    if relays:
        for off in (2, n - 2):
            rows_in(wrap(x + off), wrap(z + off))
        for relay in relays:
            far0(*relay).start()
            far1(*relay).start()

    def arrive(j, carry):
        odd = lax.rem(j, 2)
        off = (j + 1) // 2
        off = odd * off + (1 - odd) * (n - off)
        ux, uz = wrap(x + off), wrap(z + off)
        if relays:
            pl.when((j - 3) * (j - 4) > 0)(lambda: rows_in(ux, uz))
        else:
            rows_in(ux, uz)
        rcopy(tbs0.at[0], tb0.at[ux], s1_send.at[0, 0], s1_recv.at[2, ux], partner).wait_recv()
        spread0(ux)
        rcopy(tbs1.at[0], tb1.at[uz], s1_send.at[1, 0], s1_recv.at[3, uz], partner).wait_recv()
        spread1(uz)
        return carry

    lax.fori_loop(1, n, arrive, 0)

    ds[...] = dacc[...].astype(bf16).reshape(n, 2 * cap, experts)
    dr[z] = ds[z]

    def dout(v):
        return rcopy(ds.at[v], dr.at[z], d_send.at[v], d_recv.at[z], at_z(v))

    for d in order:
        dout(wrap(z + d)).start()

    w_in.wait()
    w_out = rcopy(w_v, wp_v, x_send.at[0], x_recv.at[0], partner)
    w_out.start()

    hs_in.wait()
    tile = ch * n // 4

    def gmul(i, carry):
        l = i // 4
        at = pl.multiple_of(i * tile, tile)
        g_v[pl.ds(at, tile), :] = lax.dot_general(
            hs_v[pl.ds(at, tile), :], w_v[l], (((1,), (1,)), ((), ())), preferred_element_type=f32)
        return carry

    lax.fori_loop(0, 8, gmul, 0)

    ex0 = rcopy(r0.at[:, :, 1 - c], e0, x_send.at[1], x_recv.at[1], partner)
    ex1 = rcopy(r1.at[:, 1 - c], e1, x_send.at[2], x_recv.at[2], partner)

    def give0(v):
        rcopy(r0.at[v, :, 1 - c], e0.at[v], x_send.at[1], x_recv.at[1], partner).start()

    give0(z)
    for d in order:
        vx = wrap(x + d)
        rcopy(sb1.at[0], r1.at[vx // 2, lax.rem(vx, 2)], s2_send.at[1, 0], s2_recv.at[1, vx], partner).wait_recv()
    ex1.start()
    for d in order:
        vz = wrap(z + d)
        rcopy(sb0.at[0], r0.at[vz], s2_send.at[0, 0], s2_recv.at[0, vz], partner).wait_recv()
        give0(vz)

    def scores():
        eye = iota((ch, ch), 0) == iota((ch, ch), 1)
        for l in range(2):
            for xb in range(n):
                q = l * n * ch + xb * ch
                a0 = r0[:, xb // 2, xb % 2, l].reshape(ch, half).astype(f32)
                a1 = r1[xb // 2, xb % 2, :, l].reshape(ch, half).astype(f32)
                s = a0 * g_v[q:q + ch, :half] + a1 * g_v[q:q + ch, half:]
                s = jnp.sum(s, axis=1, keepdims=True)
                s_v[l * n + xb:l * n + xb + 1, :] = jnp.sum(jnp.where(eye, s, 0.0), axis=0, keepdims=True)

    def partial(chunk, d, own, other):
        l, xh = chunk // hn, lax.rem(chunk, hn)
        zs = pl.ds(d * hn, hn)
        if own:
            mine = jnp.concatenate(
                [r0[zs, xh, c, l].reshape(rows, half), r1[xh, c, zs, l].reshape(rows, half)], axis=1)
        if other:
            their = jnp.concatenate(
                [e0[zs, xh, l].reshape(rows, half), e1[xh, zs, l].reshape(rows, half)], axis=1)
        step = width // 4
        for j in range(4):
            cols = slice(j * step, (j + 1) * step)
            total = jnp.dot(mine, w_v[l, :, cols], preferred_element_type=f32) if own else acc[d, :, cols]
            if other:
                total = total + jnp.dot(their, wp_v[l, :, cols], preferred_element_type=f32)
            acc[d, :, cols] = total

    def hop(s, d, i, j):
        to = at_y(wrap(y + 1)) if d == 0 else at_y(wrap(y - 1 + n))
        return rcopy(snd.at[d, s, i, j], rcv.at[d, s, i, j], r_send.at[d, s, i, j], r_recv.at[d, s, i, j], to)

    def at_step(s, d):
        return wrap(y - 1 - s + n) if d == 0 else wrap(y + 1 + s)

    def ring(s):
        if s == 0:
            for d in range(2):
                partial(at_step(0, d), d, True, False)
            score_a()
            w_out.wait_recv()
            ex1.wait_recv()
            ex0.wait_recv()
            for d in range(2):
                partial(at_step(0, d), d, False, True)
        else:
            for d in range(2):
                partial(at_step(s, d), d, True, True)
        for i in range(hn):
            for j in range(parts):
                for d in range(2):
                    val = acc[d, i * cap:(i + 1) * cap, j * wide_part:(j + 1) * wide_part]
                    if s > 0:
                        hop(s - 1, d, i, j).wait_recv()
                        val = val + rcv[d, s - 1, i, j].astype(f32)
                    snd[d, s, i, j] = val.astype(bf16)
                    hop(s, d, i, j).start()

    def aout(v):
        return rcopy(s_v, sa.at[z], a_send.at[v], a_recv.at[z], at_z(v))

    def bout(v):
        return rcopy(bs.at[v], sc.at[x], b_send.at[v], b_recv.at[x], at_x(v))

    def yout(v):
        return rcopy(q_y, q_r.at[y], y_send.at[v], y_recv.at[y], at_y(v))

    qx = rcopy(q_s, q_c, x_send.at[3], x_recv.at[3], partner)

    def score_a():
        scores()
        sa[z] = s_v[...]
        for d in order:
            aout(wrap(z + d)).start()

    def score_b():
        for d in order:
            v = wrap(z + d)
            rcopy(s_v, sa.at[v], a_send.at[0], a_recv.at[v], partner).wait_recv()
        for v in range(n):
            for l in range(2):
                for xb in range(n):
                    bs[xb, v * 2 + l:v * 2 + l + 1, :] = sa[v, l * n + xb:l * n + xb + 1, :]
        sc[x] = bs[x]
        for d in order:
            bout(wrap(x + d)).start()

    def score_c():
        for d in order:
            v = wrap(x + d)
            rcopy(bs.at[0], sc.at[v], b_send.at[0], b_recv.at[v], partner).wait_recv()
        ct[...] = sc[...].reshape(experts, ch).T
        q_s[...] = ct[pl.ds(pl.multiple_of(z * cap, cap), cap), :]
        qx.start()

    def score_d():
        qx.wait_recv()
        q_y[...] = q_s[...] + q_c[...]
        q_r[y] = q_y[...]
        for d in order:
            yout(wrap(y + d)).start()

    def finish():
        rw_in.wait()
        for d in order:
            v = wrap(y + d)
            rcopy(q_y, q_r.at[v], y_send.at[0], y_recv.at[v], partner).wait_recv()
        total = q_r[0]
        for v in range(1, n):
            total = total + q_r[v]
        codes = code_v[...].T
        pair = jnp.zeros((tokens, experts), f32)
        for r in range(cap):
            pair += jnp.where(codes == float(r), total[r:r + 1, :], 0.0)
        probs = prob_v[...].T
        mean = jnp.sum(probs * pair, axis=1, keepdims=True) / route_scale
        grad = (probs * (1.0 - jax.nn.sigmoid(lg_v[...])) * (pair - mean)).astype(bf16)
        ig_ref[...] = jnp.dot(grad, rw_v[...], preferred_element_type=f32).astype(bf16)

    def probs_in():
        for d in order:
            v = wrap(z + d)
            rcopy(ds.at[0], dr.at[v], d_send.at[0], d_recv.at[v], partner).wait_recv()
        mine = dr[...].reshape(n * 2 * cap, experts).astype(f32)
        shape = (n * 2 * cap, experts)
        keep = iota(shape, 1) % ge == z * 2 + iota(shape, 0) // cap % 2
        mine = jnp.where(keep, mine, 0.0).astype(bf16)
        wide = (experts, n * half)
        pick = (iota(wide, 0) // ge == iota(wide, 1) // half).astype(f32).astype(bf16)
        pb[...] = jnp.dot(mine, pick, preferred_element_type=f32).reshape(n, 2, cap, n * half)

    def scale(l):
        for xb in range(n):
            p = pb[:, l, :, xb * half:(xb + 1) * half].reshape(ch, half)
            a0 = r0[:, xb // 2, xb % 2, l].reshape(ch, half).astype(f32)
            a1 = r1[xb // 2, xb % 2, :, l].reshape(ch, half).astype(f32)
            sr[l, xb * ch:(xb + 1) * ch, :half] = (p * a0).astype(bf16)
            sr[l, xb * ch:(xb + 1) * ch, half:] = (p * a1).astype(bf16)

    def grads(i):
        l, j = i // 4, i % 4
        step = width // 4
        cols = slice(j * step, (j + 1) * step)
        wg_ref[l, :, cols] = lax.dot_general(
            sr[l], hs_v[l * n * ch:(l + 1) * n * ch, cols], (((0,), (0,)), ((), ())),
            preferred_element_type=f32).astype(bf16)

    some = lambda f, *items: [functools.partial(f, i) for i in items]
    todo = [[probs_in], [score_b] + some(scale, 0), some(grads, 0, 1), [score_c] + some(scale, 1),
            [score_d] + some(grads, 2, 3), some(grads, 4, 5), some(grads, 6, 7) + [finish]]
    if n < 8:
        todo = [sum(todo, [])]
    for s in range(n - 1):
        ring(s)
        for work in todo[s]:
            work()
    for d in range(2):
        partial(y, d, True, True)
    mine_l, mine_x = k // n, lax.rem(k, n)
    for i in range(hn):
        for j in range(parts):
            for d in range(2):
                hop(n - 2, d, i, j).wait_recv()
                zb = d * hn + i
                p = pb[zb, mine_l, :, pl.ds(pl.multiple_of(mine_x * half, half), half)]
                for m in range(wide_part // half):
                    a, b = j * wide_part + m * half, j * wide_part + (m + 1) * half
                    val = acc[d, i * cap:(i + 1) * cap, a:b]
                    val = val + rcv[d, n - 2, i, j, :, m * half:(m + 1) * half].astype(f32)
                    hg_ref[zb * cap:(zb + 1) * cap, a:b] = (p * val).astype(bf16)

    w_out.wait_send()
    ex0.wait_send()
    ex1.wait_send()
    qx.wait_send()
    for d in order:
        vx, vz, vy = wrap(x + d), wrap(z + d), wrap(y + d)
        tab0(vx).wait_send()
        tab1(vz).wait_send()
        rcopy(sb0.at[vz], r0.at[z], s2_send.at[0, vz], s2_recv.at[0, z], partner).wait_send()
        rcopy(sb1.at[vx], r1.at[x // 2, lax.rem(x, 2)], s2_send.at[1, vx], s2_recv.at[1, x], partner).wait_send()
        dout(vz).wait_send()
        aout(vz).wait_send()
        bout(vx).wait_send()
        yout(vy).wait_send()
    for d in near:
        tok0(wrap(x + d)).wait_send()
        tok1(wrap(z + d)).wait_send()
    for relay in relays:
        far0(*relay).wait_send()
        far1(*relay).wait_send()
    for s in range(n - 1):
        for i in range(hn):
            for j in range(parts):
                for d in range(2):
                    hop(s, d, i, j).wait_send()


def put_out(wg_ref, hg_ref, ig_ref, wg_out, hg_out, ig_out, sem):
    copies = [
        pltpu.make_async_copy(src, dst, sem.at[i])
        for i, (src, dst) in enumerate(((wg_ref, wg_out), (hg_ref, hg_out), (ig_ref, ig_out)))
    ]
    for copy in copies:
        copy.start()
    for copy in copies:
        copy.wait()


def body(n, out_grad, expert_ids, router_logits, router_weight, expert_weight, hidden_saved):
    tokens, features = out_grad.shape
    half = features // 2
    experts = router_logits.shape[1]
    width = expert_weight.shape[2]
    slots = hidden_saved.shape[1]
    ge, hn, ch = 2 * n, n // 2, n * cap
    rows, parts = hn * cap, 2
    vm = pltpu.VMEM
    dma = pltpu.SemaphoreType.DMA
    scratch = [
        vm(expert_ids.shape[::-1], jnp.int32), vm((tokens, experts), f32), vm((experts, features), bf16),
        vm((slots, width), bf16), vm((2, features, width), bf16), vm((2, features, width), bf16),
        vm((2, tokens, half), bf16), vm((2, n, tokens, half), bf16),
        vm((n, 2 * ge, tokens), bf16), vm((n, ge, tokens), bf16),
        vm((n, 2 * ge, tokens), bf16), vm((n, ge, tokens), bf16),
        vm((n, n, 2, cap, half), bf16), vm((n, n, 2, cap, half), bf16),
        vm((n, hn, 2, 2, cap, half), bf16), vm((hn, 2, n, 2, cap, half), bf16),
        vm((n, hn, 2, cap, half), bf16), vm((hn, n, 2, cap, half), bf16),
        vm((ge * cap, experts), f32), vm((n, 2 * cap, experts), bf16), vm((n, 2 * cap, experts), bf16),
        vm((slots, features), f32), vm((n, 2, cap, n * half), f32), vm((2, n * ch, features), bf16),
        vm((ge, ch), f32), vm((n, ge, ch), f32), vm((n, ge, ch), f32), vm((n, ge, ch), f32),
        vm((ch, experts), f32),
        vm((cap, experts), f32), vm((cap, experts), f32), vm((cap, experts), f32), vm((n, cap, experts), f32),
        vm((2, rows, width), f32), vm((2, n - 1, hn, parts, cap, width // parts), bf16),
        vm((2, n - 1, hn, parts, cap, width // parts), bf16),
        vm((experts, tokens), f32), vm((experts, tokens), f32),
        dma((7,)), dma((2, n)), dma((2, n)), dma((4, n)), dma((2, n)), dma((2, n)), dma((n,)), dma((n,)),
        dma((4,)), dma((4,)), dma((n,)), dma((n,)), dma((n,)), dma((n,)), dma((n,)), dma((n,)),
        dma((2, n - 1, hn, parts)), dma((2, n - 1, hn, parts)),
    ]
    in_vmem = pl.BlockSpec(memory_space=pltpu.VMEM)
    in_hbm = pl.BlockSpec(memory_space=pltpu.HBM)
    weight_grad, hidden_grad, input_grad = pl.pallas_call(
        functools.partial(kernel, n),
        out_shape=(
            pltpu.VMEM((2, features, width), bf16),
            pltpu.VMEM((ch, width), bf16),
            pltpu.VMEM((tokens, features), bf16),
        ),
        in_specs=[in_hbm] * 6,
        out_specs=(in_vmem, in_vmem, in_vmem),
        scratch_shapes=scratch,
        compiler_params=pltpu.CompilerParams(collective_id=0, has_side_effects=True),
    )(out_grad, expert_ids.T, router_logits, router_weight, expert_weight, hidden_saved.reshape(slots, width))
    weight_grad, hidden_grad, input_grad = pl.pallas_call(
        put_out,
        out_shape=(
            jax.ShapeDtypeStruct((2, features, width), bf16),
            jax.ShapeDtypeStruct((ch, width), bf16),
            jax.ShapeDtypeStruct((tokens, features), bf16),
        ),
        in_specs=[pl.BlockSpec(memory_space=pl.ANY)] * 3,
        out_specs=(in_hbm, in_hbm, in_hbm),
        scratch_shapes=[dma((3,))],
        compiler_params=pltpu.CompilerParams(vmem_limit_bytes=1 << 20),
    )(weight_grad, hidden_grad, input_grad)
    return weight_grad, hidden_grad[None], input_grad


def solution(mesh):
    n = mesh.shape["ep"] // 2
    in_specs = (
        P("grp", "ep"),
        P("grp", None),
        P("grp", None),
        P(None, "ep"),
        P("grp", "ep", None),
        P("grp", None, None),
    )
    out_specs = (P("grp", "ep", None), P("grp", "ep", None), P("grp", "ep"))
    return jax.shard_map(functools.partial(body, n), mesh=mesh, in_specs=in_specs, out_specs=out_specs, check_vma=False)
```

```python
import functools
import jax
import jax.numpy as jnp
from jax import lax
from jax.experimental import pallas as pl
from jax.experimental.pallas import tpu as pltpu
from jax.sharding import PartitionSpec as P

route_scale = 2.5
cap = 16
unset = 255.0
bf16 = jnp.bfloat16
f32 = jnp.float32
MESH = pl.DeviceIdType.MESH


def iota(shape, dim):
    return lax.broadcasted_iota(jnp.int32, shape, dim)


def kernel(n, og_ref, ids_ref, lg_ref, rw_ref, ew_ref, hs_ref, wg_ref, hg_ref, ig_ref,
           ids_v, lg_v, rw_v, hs_v, w_v, wp_v, tok, tk, tbs0, tbs1, tb0, tb1, sb0, sb1, r0, r1, e0, e1,
           dacc, ds, dr, g_v, pb, sr, s_v, sa, bs, sc, ct, q_s, q_c, q_y, q_r,
           acc, snd, rcv, code_v, prob_v,
           loc_sem, t_send, s1_send, s1_recv, s2_send, s2_recv, d_send, d_recv, x_send, x_recv,
           a_send, a_recv, b_send, b_recv, y_send, y_recv, r_send, r_recv):
    tokens, half = og_ref.shape[0], og_ref.shape[1] // 2
    topk = ids_ref.shape[0]
    experts = lg_ref.shape[1]
    width = hs_v.shape[1]
    ge = 2 * n
    hn = n // 2
    ch = n * cap
    rows = hn * cap
    parts = 2
    wide_part = width // parts
    g = lax.axis_index("grp")
    k = lax.axis_index("ep")
    x, z = g // n, lax.rem(g, n)
    y, c = k // 2, lax.rem(k, 2)
    wrap = lambda v: lax.rem(v + 2 * n, n)
    at_x = lambda v: (v * n + z, k)
    at_z = lambda v: (x * n + v, k)
    at_y = lambda v: (g, v * 2 + c)
    partner = (g, y * 2 + 1 - c)

    def rcopy(src, dst, ss, rs, dev):
        return pltpu.make_async_remote_copy(
            src_ref=src, dst_ref=dst, send_sem=ss, recv_sem=rs, device_id=dev, device_id_type=MESH)

    barrier = pltpu.get_barrier_semaphore()
    for d in range(1, n):
        for at, me in ((at_x, x), (at_z, z), (at_y, y)):
            pl.semaphore_signal(barrier, inc=1, device_id=at(wrap(me + d)), device_id_type=MESH)
    pl.semaphore_signal(barrier, inc=1, device_id=partner, device_id_type=MESH)

    def local(src, dst, i):
        copy = pltpu.make_async_copy(src, dst, loc_sem.at[i])
        copy.start()
        return copy

    ids_in = local(ids_ref, ids_v, 0)
    lg_in = local(lg_ref, lg_v, 1)
    tok_in = [local(og_ref.at[:, p * half:(p + 1) * half], tok.at[p], 2 + p) for p in range(2)]
    w_in = local(ew_ref, w_v, 4)
    hs_in = local(hs_ref, hs_v, 5)
    rw_in = local(rw_ref, rw_v, 6)

    for p in range(2):
        tok_in[p].wait()
    pl.semaphore_wait(barrier, 3 * (n - 1) + 1)

    order = [d if i == 0 else n - d for d in range(1, hn + 1) for i in range(2)][: n - 1]

    def tok0(v):
        return rcopy(tok.at[0], tk.at[0, x], t_send.at[0, v], s1_recv.at[0, x], at_x(v))

    def tok1(v):
        return rcopy(tok.at[1], tk.at[1, z], t_send.at[1, v], s1_recv.at[1, z], at_z(v))

    near = order[:4]
    for d in near:
        tok0(wrap(x + d)).start()
        tok1(wrap(z + d)).start()
    tk[0, x] = tok[0]
    tk[1, z] = tok[1]

    ids_in.wait()
    row_t = iota((experts, tokens), 0)
    member = jnp.zeros((experts, tokens), f32)
    for i in range(topk):
        member += (ids_v[i:i + 1, :] == row_t).astype(f32)
    upper = (iota((tokens, tokens), 0) < iota((tokens, tokens), 1)).astype(f32).astype(bf16)
    rank = jnp.dot(member.astype(bf16), upper, preferred_element_type=f32)
    code = jnp.where(member > 0.0, rank, unset)
    code_v[...] = code
    code_t = code.astype(bf16)
    row_e, col_e = iota((experts, experts), 0), iota((experts, experts), 1)
    perm = (col_e == (row_e // 2 % n) * ge + (row_e // ge) * 2 + row_e % 2).astype(f32).astype(bf16)
    code_p = jnp.dot(perm, code_t, preferred_element_type=f32).astype(bf16)
    lg_in.wait()
    chosen = member * jax.nn.sigmoid(lg_v[...].T)
    prob = route_scale * chosen / jnp.sum(chosen, axis=0, keepdims=True)
    prob_v[...] = prob
    prob_t = prob.astype(bf16)
    for v in range(n):
        tbs0[v, 0:ge, :] = code_t[v * ge:(v + 1) * ge, :]
        tbs0[v, ge:2 * ge, :] = prob_t[v * ge:(v + 1) * ge, :]
        tbs1[v] = code_p[v * ge:(v + 1) * ge, :]
    tb0[x] = tbs0[x]
    tb1[z] = tbs1[z]

    relays = [(2, -1, 3), (2, -2, 4), (n - 2, 1, 5)] if n > 4 else []

    def far0(off, d, i):
        u = wrap(x + off)
        return rcopy(tk.at[0, u], tk.at[0, u], t_send.at[0, wrap(x + i)], s1_recv.at[0, u], at_x(wrap(x + d)))

    def far1(off, d, i):
        u = wrap(z + off)
        return rcopy(tk.at[1, u], tk.at[1, u], t_send.at[1, wrap(z + i)], s1_recv.at[1, u], at_z(wrap(z + d)))

    def rows_in(ux, uz):
        rcopy(tok.at[0], tk.at[0, ux], t_send.at[0, 0], s1_recv.at[0, ux], partner).wait_recv()
        rcopy(tok.at[1], tk.at[1, uz], t_send.at[1, 0], s1_recv.at[1, uz], partner).wait_recv()

    def tab0(v):
        return rcopy(tbs0.at[v], tb0.at[x], s1_send.at[0, v], s1_recv.at[2, x], at_x(v))

    def tab1(v):
        return rcopy(tbs1.at[v], tb1.at[z], s1_send.at[1, v], s1_recv.at[3, z], at_z(v))

    for d in order:
        tab0(wrap(x + d)).start()
        tab1(wrap(z + d)).start()

    slot_r = iota((ge, cap, tokens), 1).astype(f32)
    dacc[...] = jnp.zeros_like(dacc)

    def fill(path, table):
        hot = (table.astype(f32)[:, None, :] == slot_r).astype(f32).astype(bf16)
        hot = hot.reshape(ge * cap, tokens)
        return hot

    def out0(v, us):
        return rcopy(sb0.at[v, us], r0.at[z, us // 2, lax.rem(us, 2)], s2_send.at[0, v], s2_recv.at[0, z], at_z(v))

    def out1(v, us):
        return rcopy(sb1.at[v, us], r1.at[x // 2, lax.rem(x, 2), us], s2_send.at[1, v], s2_recv.at[1, x], at_x(v))

    def spread0(us):
        hot = fill(0, tb0[us, 0:ge, :])
        got = jnp.dot(hot, tk[0, us], preferred_element_type=f32).astype(bf16)
        sb0[:, us] = got.reshape(n, 2, cap, half)
        for d in order:
            out0(wrap(z + d), us).start()
        r0[z, us // 2, lax.rem(us, 2)] = sb0[z, us]
        table = tb0[us, ge:2 * ge, :]
        wide = jnp.concatenate([table] * n, axis=0)
        wide = jnp.where(iota((experts, tokens), 0) // ge == us, wide.astype(f32), 0.0).astype(bf16)
        dacc[...] += lax.dot_general(hot, wide, (((1,), (1,)), ((), ())), preferred_element_type=f32)

    def spread1(us):
        hot = fill(1, tb1[us])
        got = jnp.dot(hot, tk[1, us], preferred_element_type=f32).astype(bf16)
        sb1[:, us] = got.reshape(n, 2, cap, half)
        for d in order:
            out1(wrap(x + d), us).start()
        r1[x // 2, lax.rem(x, 2), us] = sb1[x, us]

    spread0(x)
    spread1(z)
    if relays:
        for off in (2, n - 2):
            rows_in(wrap(x + off), wrap(z + off))
        for relay in relays:
            far0(*relay).start()
            far1(*relay).start()

    def arrive(j, carry):
        odd = lax.rem(j, 2)
        off = (j + 1) // 2
        off = odd * off + (1 - odd) * (n - off)
        ux, uz = wrap(x + off), wrap(z + off)
        if relays:
            pl.when((j - 3) * (j - 4) > 0)(lambda: rows_in(ux, uz))
        else:
            rows_in(ux, uz)
        rcopy(tbs0.at[0], tb0.at[ux], s1_send.at[0, 0], s1_recv.at[2, ux], partner).wait_recv()
        spread0(ux)
        rcopy(tbs1.at[0], tb1.at[uz], s1_send.at[1, 0], s1_recv.at[3, uz], partner).wait_recv()
        spread1(uz)
        return carry

    lax.fori_loop(1, n, arrive, 0)

    ds[...] = dacc[...].astype(bf16).reshape(n, 2 * cap, experts)
    dr[z] = ds[z]

    def dout(v):
        return rcopy(ds.at[v], dr.at[z], d_send.at[v], d_recv.at[z], at_z(v))

    for d in order:
        dout(wrap(z + d)).start()

    w_in.wait()
    w_out = rcopy(w_v, wp_v, x_send.at[0], x_recv.at[0], partner)
    w_out.start()

    hs_in.wait()
    tile = ch * n // 4

    def gmul(i, carry):
        l = i // 4
        at = pl.multiple_of(i * tile, tile)
        g_v[pl.ds(at, tile), :] = lax.dot_general(
            hs_v[pl.ds(at, tile), :], w_v[l], (((1,), (1,)), ((), ())), preferred_element_type=f32)
        return carry

    lax.fori_loop(0, 8, gmul, 0)

    ex0 = rcopy(r0.at[:, :, 1 - c], e0, x_send.at[1], x_recv.at[1], partner)
    ex1 = rcopy(r1.at[:, 1 - c], e1, x_send.at[2], x_recv.at[2], partner)

    def give0(v):
        rcopy(r0.at[v, :, 1 - c], e0.at[v], x_send.at[1], x_recv.at[1], partner).start()

    give0(z)
    for d in order:
        vx = wrap(x + d)
        rcopy(sb1.at[0], r1.at[vx // 2, lax.rem(vx, 2)], s2_send.at[1, 0], s2_recv.at[1, vx], partner).wait_recv()
    ex1.start()
    for d in order:
        vz = wrap(z + d)
        rcopy(sb0.at[0], r0.at[vz], s2_send.at[0, 0], s2_recv.at[0, vz], partner).wait_recv()
        give0(vz)

    def scores():
        eye = iota((ch, ch), 0) == iota((ch, ch), 1)
        for l in range(2):
            for xb in range(n):
                q = l * n * ch + xb * ch
                a0 = r0[:, xb // 2, xb % 2, l].reshape(ch, half).astype(f32)
                a1 = r1[xb // 2, xb % 2, :, l].reshape(ch, half).astype(f32)
                s = a0 * g_v[q:q + ch, :half] + a1 * g_v[q:q + ch, half:]
                s = jnp.sum(s, axis=1, keepdims=True)
                s_v[l * n + xb:l * n + xb + 1, :] = jnp.sum(jnp.where(eye, s, 0.0), axis=0, keepdims=True)

    def partial(chunk, d, own, other):
        l, xh = chunk // hn, lax.rem(chunk, hn)
        zs = pl.ds(d * hn, hn)
        if own:
            mine = jnp.concatenate(
                [r0[zs, xh, c, l].reshape(rows, half), r1[xh, c, zs, l].reshape(rows, half)], axis=1)
        if other:
            their = jnp.concatenate(
                [e0[zs, xh, l].reshape(rows, half), e1[xh, zs, l].reshape(rows, half)], axis=1)
        step = width // 4
        for j in range(4):
            cols = slice(j * step, (j + 1) * step)
            total = jnp.dot(mine, w_v[l, :, cols], preferred_element_type=f32) if own else acc[d, :, cols]
            if other:
                total = total + jnp.dot(their, wp_v[l, :, cols], preferred_element_type=f32)
            acc[d, :, cols] = total

    def hop(s, d, i, j):
        to = at_y(wrap(y + 1)) if d == 0 else at_y(wrap(y - 1 + n))
        return rcopy(snd.at[d, s, i, j], rcv.at[d, s, i, j], r_send.at[d, s, i, j], r_recv.at[d, s, i, j], to)

    def at_step(s, d):
        return wrap(y - 1 - s + n) if d == 0 else wrap(y + 1 + s)

    def ring(s):
        if s == 0:
            for d in range(2):
                partial(at_step(0, d), d, True, False)
            score_a()
            w_out.wait_recv()
            ex1.wait_recv()
            ex0.wait_recv()
            for d in range(2):
                partial(at_step(0, d), d, False, True)
                for i in range(hn):
                    for j in range(parts):
                        val = acc[d, i * cap:(i + 1) * cap, j * wide_part:(j + 1) * wide_part]
                        snd[d, 0, i, j] = val.astype(bf16)
                        hop(0, d, i, j).start()
            return
        else:
            for d in range(2):
                partial(at_step(s, d), d, True, True)
        for i in range(hn):
            for j in range(parts):
                for d in range(2):
                    val = acc[d, i * cap:(i + 1) * cap, j * wide_part:(j + 1) * wide_part]
                    hop(s - 1, d, i, j).wait_recv()
                    val = val + rcv[d, s - 1, i, j].astype(f32)
                    snd[d, s, i, j] = val.astype(bf16)
                    hop(s, d, i, j).start()

    def aout(v):
        return rcopy(s_v, sa.at[z], a_send.at[v], a_recv.at[z], at_z(v))

    def bout(v):
        return rcopy(bs.at[v], sc.at[x], b_send.at[v], b_recv.at[x], at_x(v))

    def yout(v):
        return rcopy(q_y, q_r.at[y], y_send.at[v], y_recv.at[y], at_y(v))

    qx = rcopy(q_s, q_c, x_send.at[3], x_recv.at[3], partner)

    def score_a():
        scores()
        sa[z] = s_v[...]
        for d in order:
            aout(wrap(z + d)).start()

    def score_b():
        for d in order:
            v = wrap(z + d)
            rcopy(s_v, sa.at[v], a_send.at[0], a_recv.at[v], partner).wait_recv()
        for v in range(n):
            for l in range(2):
                for xb in range(n):
                    bs[xb, v * 2 + l:v * 2 + l + 1, :] = sa[v, l * n + xb:l * n + xb + 1, :]
        sc[x] = bs[x]
        for d in order:
            bout(wrap(x + d)).start()

    def score_c():
        for d in order:
            v = wrap(x + d)
            rcopy(bs.at[0], sc.at[v], b_send.at[0], b_recv.at[v], partner).wait_recv()
        ct[...] = sc[...].reshape(experts, ch).T
        q_s[...] = ct[pl.ds(pl.multiple_of(z * cap, cap), cap), :]
        qx.start()

    def score_d():
        qx.wait_recv()
        q_y[...] = q_s[...] + q_c[...]
        q_r[y] = q_y[...]
        for d in order:
            yout(wrap(y + d)).start()

    def finish():
        rw_in.wait()
        for d in order:
            v = wrap(y + d)
            rcopy(q_y, q_r.at[v], y_send.at[0], y_recv.at[v], partner).wait_recv()
        total = q_r[0]
        for v in range(1, n):
            total = total + q_r[v]
        codes = code_v[...].T
        pair = jnp.zeros((tokens, experts), f32)
        for r in range(cap):
            pair += jnp.where(codes == float(r), total[r:r + 1, :], 0.0)
        probs = prob_v[...].T
        mean = jnp.sum(probs * pair, axis=1, keepdims=True) / route_scale
        grad = (probs * (1.0 - jax.nn.sigmoid(lg_v[...])) * (pair - mean)).astype(bf16)
        ig_ref[...] = jnp.dot(grad, rw_v[...], preferred_element_type=f32).astype(bf16)

    def probs_in():
        for d in order:
            v = wrap(z + d)
            rcopy(ds.at[0], dr.at[v], d_send.at[0], d_recv.at[v], partner).wait_recv()
        mine = dr[...].reshape(n * 2 * cap, experts).astype(f32)
        shape = (n * 2 * cap, experts)
        keep = iota(shape, 1) % ge == z * 2 + iota(shape, 0) // cap % 2
        mine = jnp.where(keep, mine, 0.0).astype(bf16)
        wide = (experts, n * half)
        pick = (iota(wide, 0) // ge == iota(wide, 1) // half).astype(f32).astype(bf16)
        pb[...] = jnp.dot(mine, pick, preferred_element_type=f32).reshape(n, 2, cap, n * half)

    def scale(l):
        for xb in range(n):
            p = pb[:, l, :, xb * half:(xb + 1) * half].reshape(ch, half)
            a0 = r0[:, xb // 2, xb % 2, l].reshape(ch, half).astype(f32)
            a1 = r1[xb // 2, xb % 2, :, l].reshape(ch, half).astype(f32)
            sr[l, xb * ch:(xb + 1) * ch, :half] = (p * a0).astype(bf16)
            sr[l, xb * ch:(xb + 1) * ch, half:] = (p * a1).astype(bf16)

    def grads(i):
        l, j = i // 4, i % 4
        step = width // 4
        cols = slice(j * step, (j + 1) * step)
        wg_ref[l, :, cols] = lax.dot_general(
            sr[l], hs_v[l * n * ch:(l + 1) * n * ch, cols], (((0,), (0,)), ((), ())),
            preferred_element_type=f32).astype(bf16)

    some = lambda f, *items: [functools.partial(f, i) for i in items]
    todo = [[probs_in], [score_b] + some(scale, 0), some(grads, 0, 1), [score_c] + some(scale, 1),
            [score_d] + some(grads, 2, 3), some(grads, 4, 5), some(grads, 6, 7) + [finish]]
    if n < 8:
        todo = [sum(todo, [])]
    for s in range(n - 1):
        ring(s)
        for work in todo[s]:
            work()
    for d in range(2):
        partial(y, d, True, True)
    mine_l, mine_x = k // n, lax.rem(k, n)
    for i in range(hn):
        for j in range(parts):
            for d in range(2):
                hop(n - 2, d, i, j).wait_recv()
                zb = d * hn + i
                p = pb[zb, mine_l, :, pl.ds(pl.multiple_of(mine_x * half, half), half)]
                for m in range(wide_part // half):
                    a, b = j * wide_part + m * half, j * wide_part + (m + 1) * half
                    val = acc[d, i * cap:(i + 1) * cap, a:b]
                    val = val + rcv[d, n - 2, i, j, :, m * half:(m + 1) * half].astype(f32)
                    hg_ref[zb * cap:(zb + 1) * cap, a:b] = (p * val).astype(bf16)

    w_out.wait_send()
    ex0.wait_send()
    ex1.wait_send()
    qx.wait_send()
    for d in order:
        vx, vz, vy = wrap(x + d), wrap(z + d), wrap(y + d)
        tab0(vx).wait_send()
        tab1(vz).wait_send()
        rcopy(sb0.at[vz], r0.at[z], s2_send.at[0, vz], s2_recv.at[0, z], partner).wait_send()
        rcopy(sb1.at[vx], r1.at[x // 2, lax.rem(x, 2)], s2_send.at[1, vx], s2_recv.at[1, x], partner).wait_send()
        dout(vz).wait_send()
        aout(vz).wait_send()
        bout(vx).wait_send()
        yout(vy).wait_send()
    for d in near:
        tok0(wrap(x + d)).wait_send()
        tok1(wrap(z + d)).wait_send()
    for relay in relays:
        far0(*relay).wait_send()
        far1(*relay).wait_send()
    for s in range(n - 1):
        for i in range(hn):
            for j in range(parts):
                for d in range(2):
                    hop(s, d, i, j).wait_send()


def put_out(wg_ref, hg_ref, ig_ref, wg_out, hg_out, ig_out, sem):
    copies = [
        pltpu.make_async_copy(src, dst, sem.at[i])
        for i, (src, dst) in enumerate(((wg_ref, wg_out), (hg_ref, hg_out), (ig_ref, ig_out)))
    ]
    for copy in copies:
        copy.start()
    for copy in copies:
        copy.wait()


def body(n, out_grad, expert_ids, router_logits, router_weight, expert_weight, hidden_saved):
    tokens, features = out_grad.shape
    half = features // 2
    experts = router_logits.shape[1]
    width = expert_weight.shape[2]
    slots = hidden_saved.shape[1]
    ge, hn, ch = 2 * n, n // 2, n * cap
    rows, parts = hn * cap, 2
    vm = pltpu.VMEM
    dma = pltpu.SemaphoreType.DMA
    scratch = [
        vm(expert_ids.shape[::-1], jnp.int32), vm((tokens, experts), f32), vm((experts, features), bf16),
        vm((slots, width), bf16), vm((2, features, width), bf16), vm((2, features, width), bf16),
        vm((2, tokens, half), bf16), vm((2, n, tokens, half), bf16),
        vm((n, 2 * ge, tokens), bf16), vm((n, ge, tokens), bf16),
        vm((n, 2 * ge, tokens), bf16), vm((n, ge, tokens), bf16),
        vm((n, n, 2, cap, half), bf16), vm((n, n, 2, cap, half), bf16),
        vm((n, hn, 2, 2, cap, half), bf16), vm((hn, 2, n, 2, cap, half), bf16),
        vm((n, hn, 2, cap, half), bf16), vm((hn, n, 2, cap, half), bf16),
        vm((ge * cap, experts), f32), vm((n, 2 * cap, experts), bf16), vm((n, 2 * cap, experts), bf16),
        vm((slots, features), f32), vm((n, 2, cap, n * half), f32), vm((2, n * ch, features), bf16),
        vm((ge, ch), f32), vm((n, ge, ch), f32), vm((n, ge, ch), f32), vm((n, ge, ch), f32),
        vm((ch, experts), f32),
        vm((cap, experts), f32), vm((cap, experts), f32), vm((cap, experts), f32), vm((n, cap, experts), f32),
        vm((2, rows, width), f32), vm((2, n - 1, hn, parts, cap, width // parts), bf16),
        vm((2, n - 1, hn, parts, cap, width // parts), bf16),
        vm((experts, tokens), f32), vm((experts, tokens), f32),
        dma((7,)), dma((2, n)), dma((2, n)), dma((4, n)), dma((2, n)), dma((2, n)), dma((n,)), dma((n,)),
        dma((4,)), dma((4,)), dma((n,)), dma((n,)), dma((n,)), dma((n,)), dma((n,)), dma((n,)),
        dma((2, n - 1, hn, parts)), dma((2, n - 1, hn, parts)),
    ]
    in_vmem = pl.BlockSpec(memory_space=pltpu.VMEM)
    in_hbm = pl.BlockSpec(memory_space=pltpu.HBM)
    weight_grad, hidden_grad, input_grad = pl.pallas_call(
        functools.partial(kernel, n),
        out_shape=(
            pltpu.VMEM((2, features, width), bf16),
            pltpu.VMEM((ch, width), bf16),
            pltpu.VMEM((tokens, features), bf16),
        ),
        in_specs=[in_hbm] * 6,
        out_specs=(in_vmem, in_vmem, in_vmem),
        scratch_shapes=scratch,
        compiler_params=pltpu.CompilerParams(collective_id=0, has_side_effects=True),
    )(out_grad, expert_ids.T, router_logits, router_weight, expert_weight, hidden_saved.reshape(slots, width))
    weight_grad, hidden_grad, input_grad = pl.pallas_call(
        put_out,
        out_shape=(
            jax.ShapeDtypeStruct((2, features, width), bf16),
            jax.ShapeDtypeStruct((ch, width), bf16),
            jax.ShapeDtypeStruct((tokens, features), bf16),
        ),
        in_specs=[pl.BlockSpec(memory_space=pl.ANY)] * 3,
        out_specs=(in_hbm, in_hbm, in_hbm),
        scratch_shapes=[dma((3,))],
        compiler_params=pltpu.CompilerParams(vmem_limit_bytes=1 << 20),
    )(weight_grad, hidden_grad, input_grad)
    return weight_grad, hidden_grad[None], input_grad


def solution(mesh):
    n = mesh.shape["ep"] // 2
    in_specs = (
        P("grp", "ep"),
        P("grp", None),
        P("grp", None),
        P(None, "ep"),
        P("grp", "ep", None),
        P("grp", None, None),
    )
    out_specs = (P("grp", "ep", None), P("grp", "ep", None), P("grp", "ep"))
    return jax.shard_map(functools.partial(body, n), mesh=mesh, in_specs=in_specs, out_specs=out_specs, check_vma=False)
```
